512 devices in a mesh: groups: 2 (over y), section: 16 (over z), seq: 16 (over x, core).
Axes of the slice: x: 8, y: 2, z: 16, core: 2. Of those that a mesh axis runs over, the one named last changes fastest.
The devices are a block of a 8x8x16 slice.
Arguments:
- tokens: bfloat16 [8, 1024, 1440], P('groups', 'seq'), parts along dimension 0, may hold values from -6 to 6
- block_order: int32 [8], P('groups'), parts along dimension 0, may hold values from 0 to 3, each once
- prompt_lengths: int32 [8], P('groups'), parts along dimension 0, may hold values from 1 to 1024, 2304 in all
- norm_gain: float32 [16, 1440], P('section'), may hold values from 0.1 to 1.9
- w_query: bfloat16 [16, 1440, 2048], P('section', None, 'seq'), may hold values from -4 to 4
- w_key_value: bfloat16 [16, 1440, 512], P('section'), may hold values from -4 to 4
- w_out: bfloat16 [16, 2048, 1440], P('section', 'seq'), may hold values from -0.125 to 0.125
- sink_logits: float32 [16, 32], P('section'), may hold values from 0 to 4
Outputs:
- hidden_states: bfloat16 [16, 8, 1024, 1440], P('section', 'groups', 'seq'), parts along dimension 1
- layer_cache: bfloat16 [16, 8, 1024, 512], P('section', 'groups', 'seq'), parts along dimension 1
The draws below stay inside these ranges and needn't reach their ends.
There are 2 independent parts, one for each index of `groups`. The reference program is written for one: setup_inputs(seed, part) draws one part's arguments, and reference() takes and returns one part's arrays. A program takes and returns all parts, laid end to end along the dimension named above; an argument that names none is the same for every part. Nothing has to cross between parts.
Inputs may be any that keep to these rules, and one draw needn't show every extreme that they name: `block_order`: each of 0 to 3 exactly once. `prompt_lengths`: the longest prompt is full.
All inputs are finite; a program needn't handle non-finite values.
Results may differ from the reference program's by a relative error of at most 0.024.
Values may be sent and summed in bfloat16 or wider, within the bound.
A program may use at most 128 MiB of HBM per device.

```python
import math
import jax
import jax.numpy as jnp
import numpy as np
from jax import lax

D = 1440
HEADS = 32
KV_HEADS = 4
HEAD_DIM = 64
WIN = 128
MICRO = 4
BLOCK = 1024
LAYERS = 16


def base_keys(key):
    drawn = jax.random.normal(jax.random.fold_in(key, 7), (LAYERS, D, 2 * KV_HEADS * HEAD_DIM), jnp.float32)
    return drawn * D ** (-0.5)


def draw_w_key_value(key, part):
    return jnp.clip(base_keys(key), -4.0, 4.0).astype(jnp.bfloat16)


def draw_w_query(key, part):
    drawn = jax.random.normal(jax.random.fold_in(key, 1), (LAYERS, D, HEADS * HEAD_DIM), jnp.float32) * D ** (-0.5)
    return jnp.clip(drawn, -4.0, 4.0).astype(jnp.bfloat16)


def steps_of(own_key, extent, cuts, least, top_value):
    def one(position, blocks):
        heights = jax.random.uniform(jax.random.fold_in(jax.random.fold_in(own_key, 6), position), (blocks,), jnp.float32, least / len(cuts), top_value / len(cuts))
        return jnp.repeat(jnp.exp(heights), extent[position] // blocks).reshape((-1,) + (1,) * (len(extent) - position - 1))

    loudness = one(*cuts[0])
    for cut in cuts[1:]:
        loudness = loudness * one(*cut)
    return loudness


def length_profile(count, total, limit, lean):
    loads = [(1 << 20) // math.isqrt(rank ** lean) + 1 for rank in range(2, count + 1)]
    surplus, holding = total - limit - (count - 1), [1] * (count - 1)
    while surplus > 0:
        free = [i for i in range(count - 1) if holding[i] < limit]
        whole, left = sum([loads[i] for i in free]), surplus
        for i in free:
            addition = min(limit - holding[i], max(1, left * loads[i] // whole), surplus)
            holding[i] = holding[i] + addition
            surplus = surplus - addition
    return np.array([limit] + holding)


def uneven_parts(key, amount, total, most, lean):
    if amount == 2:
        one = jax.random.randint(key, (), max(1, total - most), min(most, total - 1) + 1)
        return jnp.stack([one, total - one])
    tallies = jnp.asarray(length_profile(amount, total, most, lean), jnp.int32)
    couples = (amount - 1) // 2
    giver, receiver = tallies[1:1 + 2 * couples:2], tallies[2:2 + 2 * couples:2]
    margin = jnp.minimum(giver - 1, most - receiver)
    shifted = jax.random.randint(jax.random.fold_in(key, 1), (couples,), 0, 1 << 20) % (margin + 1)
    tallies = tallies.at[1:1 + 2 * couples:2].set(giver - shifted).at[2:2 + 2 * couples:2].set(receiver + shifted)
    return tallies[jax.random.permutation(jax.random.fold_in(key, 2), amount)]


def noise(rng, shape, spread, reach, pieces=(), kind=jnp.bfloat16):
    level = steps_of(rng, shape, pieces, -0.22, 0.18) if pieces else 1.0
    entries = jax.random.normal(rng, shape, jnp.float32) * spread * level
    return jnp.minimum(jnp.maximum(entries, -reach), reach).astype(kind)


def setup_inputs(seed: int = 0, part: int = 0) -> dict:
    arg_keys = jax.random.split(jax.random.key(seed), 9)
    part_keys = jax.random.split(jax.random.fold_in(arg_keys[8], part), 9)
    tokens = noise(part_keys[0], (MICRO, BLOCK, D), 1.0, 6.0, ((1, 16),))
    block_order = jax.random.permutation(part_keys[1], MICRO).astype(jnp.int32)
    prompt_lengths = uneven_parts(part_keys[2], MICRO, 9 * MICRO * BLOCK // 16, BLOCK, 2).astype(jnp.int32)
    norm_gain = jnp.clip(1.0 + 0.18 * jax.random.normal(arg_keys[3], (LAYERS, D), jnp.float32), 0.1, 1.9)
    w_query = draw_w_query(jax.random.fold_in(arg_keys[8], 71), part)
    w_key_value = draw_w_key_value(jax.random.fold_in(arg_keys[8], 71), part)
    w_out = noise(arg_keys[6], (LAYERS, HEADS * HEAD_DIM, D), (HEADS * HEAD_DIM) ** -0.5, 0.125, ((0, 16), (1, 16)))
    sink_logits = jnp.clip(4.0 * jax.random.uniform(arg_keys[7], (LAYERS, HEADS), jnp.float32) ** steps_of(arg_keys[7], (LAYERS, HEADS), ((0, 16),), -0.2, 0.2), 0.0, 4.0)
    return dict(tokens=tokens, block_order=block_order, prompt_lengths=prompt_lengths, norm_gain=norm_gain, w_query=w_query, w_key_value=w_key_value, w_out=w_out, sink_logits=sink_logits)


THETA = 150000.0
EPSILON = 1e-05

def rotary(positions, head_size):
    half = head_size // 2
    freq = jnp.exp(jnp.arange(half, dtype=jnp.float32) * (-2.0 * math.log(THETA) / head_size))
    angles = positions.astype(jnp.float32)[:, None] * freq[None, :]
    return (jnp.cos(angles)[:, None, :], jnp.sin(angles)[:, None, :])

def rotate(values, cosine, sine):
    half = values.shape[-1] // 2
    first = values[..., :half]
    second = values[..., half:]
    return jnp.concatenate([first * cosine - second * sine, second * cosine + first * sine], -1)

def layer_step(hidden, gain, w_query, w_key_value, w_out, sinks, cosine, sine, allowed):
    group = HEADS // KV_HEADS
    kv_width = KV_HEADS * HEAD_DIM
    count = hidden.shape[0]
    widened = hidden.astype(jnp.float32)
    scale = lax.rsqrt(lax.optimization_barrier(jnp.mean(widened * widened, -1, keepdims=True)) + EPSILON)
    normed = (widened * scale * gain).astype(jnp.bfloat16)
    queries = jnp.dot(normed, w_query, preferred_element_type=jnp.float32).reshape(count, HEADS, HEAD_DIM)
    queries = rotate(queries, cosine, sine).astype(jnp.bfloat16)
    projected = jnp.dot(normed, w_key_value, preferred_element_type=jnp.float32)
    keys = rotate(projected[:, :kv_width].reshape(count, KV_HEADS, HEAD_DIM), cosine, sine).reshape(count, kv_width)
    cache = jnp.concatenate([keys, projected[:, kv_width:]], 1).astype(jnp.bfloat16)
    key_heads = cache[:, :kv_width].reshape(count, KV_HEADS, HEAD_DIM).astype(jnp.float32)
    value_heads = cache[:, kv_width:].reshape(count, KV_HEADS, HEAD_DIM).astype(jnp.float32)
    grouped = queries.reshape(count, KV_HEADS, group, HEAD_DIM).astype(jnp.float32)
    scores = jnp.einsum('qkgd,skd->kgqs', grouped, key_heads) * 0.125
    sink = sinks.reshape(KV_HEADS, group)[:, :, None]
    masked = jnp.where(allowed, scores, jnp.float32(-1e+30))
    top = jnp.maximum(lax.optimization_barrier(jnp.max(masked, -1)), sink)
    expo = jnp.where(allowed, jnp.exp(scores - top[..., None]), jnp.float32(0.0))
    total = lax.optimization_barrier(jnp.sum(expo, -1)) + jnp.exp(sink - top)
    weights = (expo / total[..., None]).astype(jnp.bfloat16)
    context = jnp.einsum('kgqs,skd->qkgd', weights.astype(jnp.float32), value_heads)
    context = context.reshape(count, HEADS * HEAD_DIM).astype(jnp.bfloat16)
    output = jnp.dot(context, w_out, preferred_element_type=jnp.float32)
    return ((widened + output).astype(jnp.bfloat16), cache)

def reference(tokens, block_order, prompt_lengths, norm_gain, w_query, w_key_value, w_out, sink_logits):
    positions = jnp.arange(BLOCK, dtype=jnp.int32)
    cosine, sine = rotary(positions, HEAD_DIM)
    within = (positions[None, :] <= positions[:, None]) & (positions[:, None] - positions[None, :] < WIN)
    hidden_rows = [[] for layer in range(LAYERS)]
    cache_rows = [[] for layer in range(LAYERS)]
    for slot in range(MICRO):
        block = block_order[slot]
        hidden = lax.dynamic_index_in_dim(tokens, block, 0, keepdims=False)
        length = lax.dynamic_index_in_dim(prompt_lengths, block, 0, keepdims=False)
        allowed = within & ((positions[None, :] < length) | (positions[None, :] == positions[:, None]))
        for layer in range(LAYERS):
            hidden, cache = layer_step(hidden, norm_gain[layer], w_query[layer], w_key_value[layer], w_out[layer], sink_logits[layer], cosine, sine, allowed)
            hidden_rows[layer].append(hidden)
            cache_rows[layer].append(cache)
    hidden_states = jnp.stack([jnp.stack(row) for row in hidden_rows])
    layer_cache = jnp.stack([jnp.stack(row) for row in cache_rows])
    return (hidden_states, layer_cache)
```

```python
import functools
import math

import jax
import jax.numpy as jnp
from jax import lax
from jax.experimental import pallas as pl
from jax.experimental.pallas import tpu as pltpu
from jax.sharding import PartitionSpec as P

MESH = pl.DeviceIdType.MESH
HEAD_DIM = 64
HALF = HEAD_DIM // 2
WIN = 128
TILE = 256
THETA = 150000.0
EPSILON = 1e-05
LOW = -1e30
F32 = jnp.float32
BF16 = jnp.bfloat16


def dot(a, b):
    return jnp.dot(a, b, preferred_element_type=F32)


def kernel(
    seqs, sections, micro, width,
    wq_in, wkv_in, wo_in, tok_in, cos_in, sin_in, sink_in, length_in,
    hid_out, cache_out,
    wq, wo, h, tok, kv_acc, q_acc, q, kv_own, kv_prev, ctx, o_acc, h_new, stage_h, stage_v,
    wq_recv, wq_own, wq_relay, wo_recv, wo_own, wo_relay,
    tok_send, tok_recv, h_send, h_recv, f_send, f_recv, kv_send, kv_recv, c_send, c_recv,
    oh_local, oh_send, oh_recv, oc_local, oc_send, oc_recv,
):
    chips = seqs // 2
    half_chips = chips // 2
    shards = seqs // 2
    tiles = h.shape[1] // (2 * TILE)
    ctx_tiles = shards // 2
    me = lax.axis_index("seq")
    section = lax.axis_index("section")
    x = me // 2
    c = me % 2
    other = 1 - c
    partner = {"seq": 2 * x + other}

    def chip(step, core):
        return {"seq": 2 * ((x + step + chips) % chips) + core}

    def remote(src, dst, send, recv, target):
        return pltpu.make_async_remote_copy(
            src_ref=src, dst_ref=dst, send_sem=send, recv_sem=recv, device_id=target, device_id_type=MESH
        )

    up = {"section": (section + 1) % sections}
    down = {"section": (section + sections - 1) % sections}
    barrier = pltpu.get_barrier_semaphore()
    for target in (partner, chip(1, 0), chip(1, 1), chip(-1, 0), chip(-1, 1), up, down):
        pl.semaphore_signal(barrier, inc=1, device_id=target, device_id_type=MESH)
    pl.semaphore_wait(barrier, 7)

    home = x // half_chips

    def wq_slot(index):
        return wq.at[:, pl.ds(pl.multiple_of(128 * index, 128), 128), :]

    def wo_slot(owner, core):
        return wo.at[owner, :, pl.ds(pl.multiple_of(128 * core, 128), 128)]

    mine = me - shards * home

    def own_query(which, target):
        return remote(wq_in, wq_slot(mine), wq_own.at[which], wq_recv.at[mine], target)

    def local_query():
        return pltpu.make_async_copy(wq_in, wq_slot(mine), wq_recv.at[mine])

    def own_out(half, which, target):
        return remote(wo_in.at[half], wo_slot(x, c), wo_own.at[half, which], wo_recv.at[me], target)

    def local_out():
        return pltpu.make_async_copy(wo_in.at[c], wo_slot(x, c), wo_recv.at[me])

    own_query(0, chip(1, home)).start()
    own_query(1, chip(-1, home)).start()
    for half in range(2):
        own_out(half, 0, chip(1, half)).start()
        own_out(half, 1, chip(-1, half)).start()

    @pl.when(c == home)
    def _():
        local_query().start()

    @pl.when(c != home)
    def _():
        own_query(2, partner).start()

    local_out().start()
    remote(wo_in.at[other], wo_slot(x, c), wo_own.at[other, 2], wo_recv.at[me], partner).start()

    def query_copy(index, sign):
        return remote(wq_slot(index), wq_slot(index), wq_relay.at[index], wq_recv.at[index], chip(sign, c))

    def out_copy(owner, core, sign):
        slot = wo_slot(owner, core)
        return remote(slot, slot, wo_relay.at[2 * owner + core], wo_recv.at[2 * owner + core], chip(sign, c))

    def each_query(step, sign, hops, act):
        owner = (x - sign * step + chips) % chips

        @pl.when((step <= hops) & (owner // half_chips == c))
        def _():
            for core in range(2):
                act(query_copy(2 * owner + core - shards * c, sign), step < hops)

    def each_out(step, sign, hops, act):
        owner = (x - sign * step + chips) % chips

        @pl.when(step <= hops)
        def _():
            for core in range(2):
                act(out_copy(owner, core, sign), step < hops)

    def relay(copy, more):
        copy.wait_recv()

        @pl.when(more)
        def _():
            copy.start()

    def settle(copy, more):
        @pl.when(more)
        def _():
            copy.wait_send()

    def each_step(act):
        def body(step, carry):
            each_query(step, 1, half_chips, act)
            each_query(step, -1, half_chips - 1, act)
            each_out(step, -1, half_chips, act)
            each_out(step, 1, half_chips - 1, act)
            return carry

        lax.fori_loop(1, half_chips + 1, body, 0)

    rows = pl.ds(pl.multiple_of(64 * c, 64), 64)
    other_rows = pl.ds(pl.multiple_of(64 * other, 64), 64)

    def tok_remote():
        return remote(tok_in, tok.at[:, rows, :], tok_send, tok_recv.at[1], partner)

    def tok_local():
        return pltpu.make_async_copy(tok_in, tok.at[:, rows, :], tok_recv.at[0])

    @pl.when(section == 0)
    def _():
        tok_remote().start()
        tok_local().start()
        tok_local().wait()
        tok_remote().wait()

        def turn(slot, carry):
            for k in range(2 * tiles):
                piece = tok[slot, :, TILE * k : TILE * (k + 1)].astype(F32)
                h[slot, TILE * k : TILE * (k + 1), :] = piece.T.astype(BF16)
            return carry

        lax.fori_loop(0, micro, turn, 0)

    @pl.when(x == 0)
    def _():
        kv_prev[...] = jnp.zeros_like(kv_prev)

    each_step(relay)
    own_slot = wq_slot(2 * (x % half_chips))

    @pl.when(c == home)
    def _():
        for core in range(2):
            index = 2 * x + core - shards * c
            pltpu.make_async_copy(wq_in, wq_slot(index), wq_recv.at[index]).wait()

    for core in range(2):
        pltpu.make_async_copy(wo_in.at[0], wo_slot(x, core), wo_recv.at[2 * x + core]).wait()

    def h_tile(slot, k):
        return h.at[slot, pl.ds(pl.multiple_of(TILE * k, TILE), TILE), :]

    def pass_on(slot, k):
        return remote(h_new.at[slot, k], h_tile(slot, tiles * c + k), h_send.at[slot, k], h_recv.at[slot, k], up)

    def forward(slot, k, core):
        piece = h_tile(slot, tiles * core + k)
        return remote(piece, piece, f_send.at[slot, k], f_recv.at[slot, k], partner)

    def kv_copy(slot, which):
        return remote(
            kv_own.at[slot, which], kv_prev.at[slot, which], kv_send.at[slot, which], kv_recv.at[slot, which],
            chip(1, c),
        )

    def ctx_tile(core, m):
        return pl.ds(pl.multiple_of(TILE * (ctx_tiles * core + m), TILE), TILE)

    def ctx_copy(slot, core, m):
        piece = ctx.at[slot, ctx_tile(core, m), :]
        return remote(piece, piece, c_send.at[slot, m], c_recv.at[slot, m], partner)

    def hid_columns(core, k):
        return pl.ds(pl.multiple_of(TILE * (tiles * core + k), TILE), TILE)

    def hid_local(slot, k):
        return pltpu.make_async_copy(
            stage_h.at[slot, k, rows, :], hid_out.at[slot, :, hid_columns(c, k)], oh_local.at[slot, k]
        )

    def hid_remote(slot, k, core):
        return remote(
            stage_h.at[slot, k, other_rows, :], hid_out.at[slot, :, hid_columns(core, k)],
            oh_send.at[slot, k], oh_recv.at[slot, k], partner,
        )

    def cache_columns(core, which):
        return pl.ds(pl.multiple_of(256 * which + 128 * core, 128), 128)

    def cache_source(slot, which, span):
        return kv_own.at[slot, 0, span, :] if which == 0 else stage_v.at[slot, span, :]

    def cache_local(slot, which):
        return pltpu.make_async_copy(
            cache_source(slot, which, rows), cache_out.at[slot, :, cache_columns(c, which)], oc_local.at[slot, which]
        )

    def cache_remote(slot, which, core):
        return remote(
            cache_source(slot, which, other_rows), cache_out.at[slot, :, cache_columns(core, which)],
            oc_send.at[slot, which], oc_recv.at[slot, which], partner,
        )

    key = lax.broadcasted_iota(jnp.int32, (WIN, 128), 0)
    token = lax.broadcasted_iota(jnp.int32, (WIN, 128), 1)
    lower = key <= token
    lower_pair = jnp.concatenate([lower.astype(jnp.int32)] * 2, 1) == 1

    def one_slot(slot, carry):
        length = length_in[slot]
        allowed_own = (WIN * x + key < length) | (key == token)
        allowed_prev = (WIN * x - WIN + key < length) & (x > 0)
        bias = jnp.where(lower, jnp.where(allowed_own, 0.0, LOW), jnp.where(allowed_prev, 0.0, LOW))
        bias = jnp.concatenate([bias, bias], 1)

        kv_acc[...] = jnp.zeros_like(kv_acc)
        q_acc[...] = jnp.zeros_like(q_acc)
        squares = jnp.zeros((8, 128), F32)
        for k in range(tiles):
            for own in (True, False):
                core = c if own else other
                kt = tiles * core + k

                @pl.when(section > 0)
                def _():
                    if own:
                        pass_on(slot, k).wait_recv()
                        forward(slot, k, c).start()
                    else:
                        forward(slot, k, other).wait_recv()

                piece = h[slot, pl.ds(pl.multiple_of(TILE * kt, TILE), TILE), :]
                wide = piece.astype(F32)
                squares = squares + jnp.sum((wide * wide).reshape(TILE // 8, 8, 128), 0)
                kv_acc[...] += dot(wkv_in[kt], piece)
                if k < tiles - 1 or own:
                    q_acc[...] += dot(wq[kt], piece)
        scale = lax.rsqrt(jnp.sum(squares, 0, keepdims=True) * (1.0 / width) + EPSILON)
        cosine = cos_in[...] * scale
        sine = sin_in[...] * scale

        def rotate(first, second):
            return jnp.concatenate([first * cosine - second * sine, second * cosine + first * sine], 0)

        keys = jnp.concatenate(
            [rotate(kv_acc[64 * g : 64 * g + 32, :], kv_acc[64 * g + 32 : 64 * g + 64, :]) for g in range(2)], 0
        )
        kv_own[slot, 0] = keys.T.astype(BF16)

        @pl.when(x < chips - 1)
        def _():
            kv_copy(slot, 0).start()

        kv_own[slot, 1] = (kv_acc[128:256, :] * scale).astype(BF16)

        @pl.when(x < chips - 1)
        def _():
            kv_copy(slot, 1).start()

        q_acc[...] += dot(wq[kt], piece)
        for i in range(q.shape[0] // HEAD_DIM):
            first = q_acc[HEAD_DIM * i : HEAD_DIM * i + HALF, :]
            second = q_acc[HEAD_DIM * i + HALF : HEAD_DIM * (i + 1), :]
            q[HEAD_DIM * i : HEAD_DIM * (i + 1), :] = rotate(first, second).astype(BF16)

        cache_local(slot, 0).start()
        cache_remote(slot, 0, c).start()

        @pl.when(x > 0)
        def _():
            kv_copy(slot, 0).wait_recv()
            kv_copy(slot, 1).wait_recv()

        blank = jnp.zeros((HEAD_DIM, 256), BF16)
        ones = jnp.ones((16, 256), BF16)
        for p in range(shards):
            g = p // (shards // 2)
            pair = jnp.concatenate([q[128 * p : 128 * p + 64, :], q[128 * p + 64 : 128 * p + 128, :]], 1)
            pair = jnp.concatenate([pair, blank] if g == 0 else [blank, pair], 0)
            both = dot(jnp.concatenate([kv_own[slot, 0], kv_prev[slot, 0]], 0), pair)
            scores = jnp.where(lower_pair, both[:WIN], both[WIN:]) + bias
            sink = jnp.concatenate([sink_in[2 * p : 2 * p + 1, :], sink_in[2 * p + 1 : 2 * p + 2, :]], 1)
            top = jnp.maximum(jnp.max(scores, 0, keepdims=True), sink)
            expo = jnp.exp(scores - top)
            weights = jnp.concatenate(
                [jnp.where(lower_pair, expo, 0.0).astype(BF16), jnp.where(lower_pair, 0.0, expo).astype(BF16)], 0
            )
            values = jnp.concatenate(
                [kv_own[slot, 1, 64 * g : 64 * g + 64, :], kv_prev[slot, 1, 64 * g : 64 * g + 64, :]], 1
            )
            mixed = dot(jnp.concatenate([values, ones], 0), weights)
            total = mixed[HEAD_DIM : HEAD_DIM + 1, :] + jnp.exp(sink - top)
            context = (mixed[:HEAD_DIM, :] * (1.0 / total)).astype(BF16)
            base = pl.multiple_of(128 * shards * c + 128 * p, 128)
            ctx[slot, pl.ds(base, 64), :] = context[:, :128]
            ctx[slot, pl.ds(base + 64, 64), :] = context[:, 128:]
            if p % 2 == 1:
                ctx_copy(slot, c, p // 2).start()

        for k in range(tiles):
            total = jnp.zeros((TILE, 128), F32)
            for m in range(ctx_tiles):
                total = total + dot(wo[ctx_tiles * c + m, TILE * k : TILE * (k + 1), :], ctx[slot, ctx_tile(c, m), :])
            o_acc[TILE * k : TILE * (k + 1), :] = total
        for m in range(ctx_tiles):
            ctx_copy(slot, other, m).wait_recv()
        for k in range(tiles):
            total = o_acc[TILE * k : TILE * (k + 1), :]
            for m in range(ctx_tiles):
                total = total + dot(
                    wo[ctx_tiles * other + m, TILE * k : TILE * (k + 1), :], ctx[slot, ctx_tile(other, m), :]
                )
            row = pl.multiple_of(TILE * (tiles * c + k), TILE)
            h_new[slot, k] = (h[slot, pl.ds(row, TILE), :].astype(F32) + total).astype(BF16)

            @pl.when(section < sections - 1)
            def _():
                pass_on(slot, k).start()

        stage_v[slot] = kv_own[slot, 1].astype(F32).T.astype(BF16)
        cache_local(slot, 1).start()
        cache_remote(slot, 1, c).start()
        for k in range(tiles):
            stage_h[slot, k] = h_new[slot, k].astype(F32).T.astype(BF16)
            hid_local(slot, k).start()
            hid_remote(slot, k, c).start()
        return carry

    lax.fori_loop(0, micro, one_slot, 0)

    def finish(slot, carry):
        for k in range(tiles):
            hid_local(slot, k).wait()
            hid_remote(slot, k, other).wait_recv()
            hid_remote(slot, k, c).wait_send()

            @pl.when(section < sections - 1)
            def _():
                pass_on(slot, k).wait_send()

            @pl.when(section > 0)
            def _():
                forward(slot, k, c).wait_send()

        for which in range(2):
            cache_local(slot, which).wait()
            cache_remote(slot, which, other).wait_recv()
            cache_remote(slot, which, c).wait_send()

            @pl.when(x < chips - 1)
            def _():
                kv_copy(slot, which).wait_send()

        for m in range(ctx_tiles):
            ctx_copy(slot, c, m).wait_send()
        return carry

    lax.fori_loop(0, micro, finish, 0)
    each_step(settle)
    own_query(0, chip(1, home)).wait_send()
    own_query(1, chip(-1, home)).wait_send()
    for half in range(2):
        own_out(half, 0, chip(1, half)).wait_send()
        own_out(half, 1, chip(-1, half)).wait_send()

    @pl.when(c != home)
    def _():
        own_query(2, partner).wait_send()

    remote(wo_in.at[other], wo_slot(x, c), wo_own.at[other, 2], wo_recv.at[me], partner).wait_send()


def per_device(seqs, sections, tokens, block_order, prompt_lengths, norm_gain, w_query, w_key_value, w_out, sinks):
    micro, rows, width = tokens.shape
    padded = -(-width // (2 * TILE)) * 2 * TILE
    tiles = padded // (2 * TILE)
    shards = seqs // 2
    me = lax.axis_index("seq")
    core = me % 2
    extra = padded - width
    gain = norm_gain[0][:, None]
    kv_width = w_key_value.shape[2] // 2

    def turned(weight):
        weight = jnp.pad(weight.astype(BF16), ((0, extra), (0, 0)))
        return weight.reshape(padded // TILE, TILE, weight.shape[1]).transpose(0, 2, 1)

    wq = turned(w_query[0].astype(F32) * (gain * (HEAD_DIM**-0.5)))
    pair = jnp.concatenate(
        [
            lax.dynamic_slice_in_dim(w_key_value[0], core * (kv_width // 2), kv_width // 2, 1),
            lax.dynamic_slice_in_dim(w_key_value[0], kv_width + core * (kv_width // 2), kv_width // 2, 1),
        ],
        1,
    )
    wkv = turned(pair.astype(F32) * gain)
    wo = jnp.pad(w_out[0], ((0, 0), (0, extra))).reshape(w_out.shape[1], 2, padded // 2).transpose(1, 2, 0)
    tok = jnp.pad(tokens[block_order], ((0, 0), (0, 0), (0, extra)))
    lengths = prompt_lengths[block_order]
    freq = jnp.exp(jnp.arange(HALF, dtype=F32) * (-2.0 * math.log(THETA) / HEAD_DIM))
    positions = (me // 2) * (2 * rows) + jnp.arange(2 * rows, dtype=jnp.int32)
    angles = freq[:, None] * positions.astype(F32)[None, :]
    heads = 2 * shards
    sink = lax.dynamic_slice_in_dim(sinks[0], core * heads, heads, 0)
    sink = jnp.broadcast_to(sink[:, None], (heads, 128))

    vmem = pl.BlockSpec(memory_space=pltpu.VMEM)
    dma = pltpu.SemaphoreType.DMA
    cells = 64 * heads
    hidden, cache = pl.pallas_call(
        functools.partial(kernel, seqs, sections, micro, width),
        out_shape=(
            jax.ShapeDtypeStruct((micro, rows, padded), BF16),
            jax.ShapeDtypeStruct((micro, rows, 2 * kv_width), BF16),
        ),
        in_specs=[vmem] * 7 + [pl.BlockSpec(memory_space=pltpu.SMEM)],
        out_specs=(pl.BlockSpec(memory_space=pl.ANY), pl.BlockSpec(memory_space=pl.ANY)),
        scratch_shapes=[
            pltpu.VMEM((2 * tiles, cells, TILE), BF16),
            pltpu.VMEM((shards, tiles * TILE, TILE), BF16),
            pltpu.VMEM((micro, padded, 128), BF16),
            pltpu.VMEM((micro, 128, padded), BF16),
            pltpu.VMEM((256, 128), F32),
            pltpu.VMEM((cells, 128), F32),
            pltpu.VMEM((cells, 128), BF16),
            pltpu.VMEM((micro, 2, 128, 128), BF16),
            pltpu.VMEM((micro, 2, 128, 128), BF16),
            pltpu.VMEM((micro, 2 * cells, 128), BF16),
            pltpu.VMEM((tiles * TILE, 128), F32),
            pltpu.VMEM((micro, tiles, TILE, 128), BF16),
            pltpu.VMEM((micro, tiles, 128, TILE), BF16),
            pltpu.VMEM((micro, 128, 128), BF16),
            dma((shards,)), dma((3,)), dma((shards,)),
            dma((seqs,)), dma((2, 3)), dma((seqs,)),
            dma, dma((2,)),
            dma((micro, tiles)), dma((micro, tiles)),
            dma((micro, tiles)), dma((micro, tiles)),
            dma((micro, 2)), dma((micro, 2)),
            dma((micro, shards // 2)), dma((micro, shards // 2)),
            dma((micro, tiles)), dma((micro, tiles)), dma((micro, tiles)),
            dma((micro, 2)), dma((micro, 2)), dma((micro, 2)),
        ],
        compiler_params=pltpu.CompilerParams(
            collective_id=0, has_side_effects=True, vmem_limit_bytes=50 * 1024 * 1024
        ),
    )(wq, wkv, wo, tok, jnp.cos(angles), jnp.sin(angles), sink, lengths)
    return hidden[None, :, :, :width], cache[None]


def solution(mesh):
    in_specs = (
        P("groups", "seq", None),
        P("groups"),
        P("groups"),
        P("section", None),
        P("section", None, "seq"),
        P("section", None, None),
        P("section", "seq", None),
        P("section", None),
    )
    out_specs = (P("section", "groups", "seq", None), P("section", "groups", "seq", None))
    body = functools.partial(per_device, mesh.shape["seq"], mesh.shape["section"])
    return jax.shard_map(body, mesh=mesh, in_specs=in_specs, out_specs=out_specs, check_vma=False)
```

```python
import functools
import math

import jax
import jax.numpy as jnp
from jax import lax
from jax.experimental import pallas as pl
from jax.experimental.pallas import tpu as pltpu
from jax.sharding import PartitionSpec as P

MESH = pl.DeviceIdType.MESH
HEAD_DIM = 64
HALF = HEAD_DIM // 2
WIN = 128
TILE = 256
THETA = 150000.0
EPSILON = 1e-05
LOW = -1e30
LOG2E = math.log2(math.e)
F32 = jnp.float32
BF16 = jnp.bfloat16


def dot(a, b):
    return jnp.dot(a, b, preferred_element_type=F32)


def kernel(
    seqs, sections, micro, width,
    wq_in, wkv_in, wo_in, tok_in, cos_in, sin_in, sink_in, length_in,
    hid_out, cache_out,
    wq, wo, h, tok, kv_acc, q_acc, q, kv_own, kv_prev, ctx, o_acc, h_new, stage_h, stage_v,
    wq_recv, wq_own, wq_relay, wo_recv, wo_own, wo_relay,
    tok_send, tok_recv, h_send, h_recv, f_send, f_recv, kv_send, kv_recv, c_send, c_recv,
    oh_local, oh_send, oh_recv, oc_local, oc_send, oc_recv,
):
    chips = seqs // 2
    half_chips = chips // 2
    shards = seqs // 2
    tiles = h.shape[1] // (2 * TILE)
    ctx_tiles = shards // 2
    me = lax.axis_index("seq")
    section = lax.axis_index("section")
    x = me // 2
    c = me % 2
    other = 1 - c
    partner = {"seq": 2 * x + other}

    def chip(step, core):
        return {"seq": 2 * ((x + step + chips) % chips) + core}

    def remote(src, dst, send, recv, target):
        return pltpu.make_async_remote_copy(
            src_ref=src, dst_ref=dst, send_sem=send, recv_sem=recv, device_id=target, device_id_type=MESH
        )

    up = {"section": (section + 1) % sections}
    down = {"section": (section + sections - 1) % sections}
    barrier = pltpu.get_barrier_semaphore()
    for target in (partner, chip(1, 0), chip(1, 1), chip(-1, 0), chip(-1, 1), up, down):
        pl.semaphore_signal(barrier, inc=1, device_id=target, device_id_type=MESH)
    pl.semaphore_wait(barrier, 7)

    home = x // half_chips

    def wq_slot(index):
        return wq.at[:, pl.ds(pl.multiple_of(128 * index, 128), 128), :]

    def wo_slot(owner, core):
        return wo.at[owner, :, pl.ds(pl.multiple_of(128 * core, 128), 128)]

    mine = me - shards * home

    def own_query(which, target):
        return remote(wq_in, wq_slot(mine), wq_own.at[which], wq_recv.at[mine], target)

    def local_query():
        return pltpu.make_async_copy(wq_in, wq_slot(mine), wq_recv.at[mine])

    def own_out(half, which, target):
        return remote(wo_in.at[half], wo_slot(x, c), wo_own.at[half, which], wo_recv.at[me], target)

    def local_out():
        return pltpu.make_async_copy(wo_in.at[c], wo_slot(x, c), wo_recv.at[me])

    own_query(0, chip(1, home)).start()
    own_query(1, chip(-1, home)).start()
    for half in range(2):
        own_out(half, 0, chip(1, half)).start()
        own_out(half, 1, chip(-1, half)).start()

    @pl.when(c == home)
    def _():
        local_query().start()

    @pl.when(c != home)
    def _():
        own_query(2, partner).start()

    local_out().start()
    remote(wo_in.at[other], wo_slot(x, c), wo_own.at[other, 2], wo_recv.at[me], partner).start()

    def query_copy(index, sign):
        return remote(wq_slot(index), wq_slot(index), wq_relay.at[index], wq_recv.at[index], chip(sign, c))

    def out_copy(owner, core, sign):
        slot = wo_slot(owner, core)
        return remote(slot, slot, wo_relay.at[2 * owner + core], wo_recv.at[2 * owner + core], chip(sign, c))

    def each_query(step, sign, hops, act):
        owner = (x - sign * step + chips) % chips

        @pl.when((step <= hops) & (owner // half_chips == c))
        def _():
            for core in range(2):
                act(query_copy(2 * owner + core - shards * c, sign), step < hops)

    def each_out(step, sign, hops, act):
        owner = (x - sign * step + chips) % chips

        @pl.when(step <= hops)
        def _():
            for core in range(2):
                act(out_copy(owner, core, sign), step < hops)

    def relay(copy, more):
        copy.wait_recv()

        @pl.when(more)
        def _():
            copy.start()

    def settle(copy, more):
        @pl.when(more)
        def _():
            copy.wait_send()

    def each_step(act):
        def body(step, carry):
            each_query(step, 1, half_chips, act)
            each_query(step, -1, half_chips - 1, act)
            each_out(step, -1, half_chips, act)
            each_out(step, 1, half_chips - 1, act)
            return carry

        lax.fori_loop(1, half_chips + 1, body, 0)

    rows = pl.ds(pl.multiple_of(64 * c, 64), 64)
    other_rows = pl.ds(pl.multiple_of(64 * other, 64), 64)

    def tok_remote():
        return remote(tok_in, tok.at[:, rows, :], tok_send, tok_recv.at[1], partner)

    def tok_local():
        return pltpu.make_async_copy(tok_in, tok.at[:, rows, :], tok_recv.at[0])

    @pl.when(section == 0)
    def _():
        tok_remote().start()
        tok_local().start()
        tok_local().wait()
        tok_remote().wait()

        def turn(slot, carry):
            for k in range(2 * tiles):
                piece = tok[slot, :, TILE * k : TILE * (k + 1)].astype(F32)
                h[slot, TILE * k : TILE * (k + 1), :] = piece.T.astype(BF16)
            return carry

        lax.fori_loop(0, micro, turn, 0)

    @pl.when(section > 0)
    def _():
        h[:, width:, :] = jnp.zeros((micro, h.shape[1] - width, 128), BF16)

    @pl.when(x == 0)
    def _():
        kv_prev[...] = jnp.zeros_like(kv_prev)

    each_step(relay)

    @pl.when(c == home)
    def _():
        for core in range(2):
            index = 2 * x + core - shards * c
            pltpu.make_async_copy(wq_in, wq_slot(index), wq_recv.at[index]).wait()

    for core in range(2):
        pltpu.make_async_copy(wo_in.at[0], wo_slot(x, core), wo_recv.at[2 * x + core]).wait()

    short = width - (2 * tiles - 1) * TILE

    def sized(core, k, act):
        if k < tiles - 1 or short == TILE:
            act(TILE)
        else:

            @pl.when(core == 0)
            def _():
                act(TILE)

            @pl.when(core == 1)
            def _():
                act(short)

    def h_tile(slot, k, size):
        return h.at[slot, pl.ds(pl.multiple_of(TILE * k, TILE), size), :]

    def pass_on(slot, k, size):
        return remote(
            h_new.at[slot, k, :size, :], h_tile(slot, tiles * c + k, size), h_send.at[slot, k], h_recv.at[slot, k], up
        )

    def forward(slot, k, core, size):
        piece = h_tile(slot, tiles * core + k, size)
        return remote(piece, piece, f_send.at[slot, k], f_recv.at[slot, k], partner)

    def kv_copy(slot, which):
        return remote(
            kv_own.at[slot, which], kv_prev.at[slot, which], kv_send.at[slot, which], kv_recv.at[slot, which],
            chip(1, c),
        )

    def ctx_tile(core, m):
        return pl.ds(pl.multiple_of(TILE * (ctx_tiles * core + m), TILE), TILE)

    def ctx_copy(slot, core, m):
        piece = ctx.at[slot, ctx_tile(core, m), :]
        return remote(piece, piece, c_send.at[slot, m], c_recv.at[slot, m], partner)

    def hid_columns(core, k):
        return pl.ds(pl.multiple_of(TILE * (tiles * core + k), TILE), TILE)

    def hid_local(slot, k):
        return pltpu.make_async_copy(
            stage_h.at[slot, k, rows, :], hid_out.at[slot, :, hid_columns(c, k)], oh_local.at[slot, k]
        )

    def hid_remote(slot, k, core):
        return remote(
            stage_h.at[slot, k, other_rows, :], hid_out.at[slot, :, hid_columns(core, k)],
            oh_send.at[slot, k], oh_recv.at[slot, k], partner,
        )

    def cache_columns(core, which):
        return pl.ds(pl.multiple_of(256 * which + 128 * core, 128), 128)

    def cache_source(slot, which, span):
        return kv_own.at[slot, 0, span, :] if which == 0 else stage_v.at[slot, span, :]

    def cache_local(slot, which):
        return pltpu.make_async_copy(
            cache_source(slot, which, rows), cache_out.at[slot, :, cache_columns(c, which)], oc_local.at[slot, which]
        )

    def cache_remote(slot, which, core):
        return remote(
            cache_source(slot, which, other_rows), cache_out.at[slot, :, cache_columns(core, which)],
            oc_send.at[slot, which], oc_recv.at[slot, which], partner,
        )

    key = lax.broadcasted_iota(jnp.int32, (WIN, 128), 0)
    token = lax.broadcasted_iota(jnp.int32, (WIN, 128), 1)
    lower = key <= token
    lower_pair = jnp.concatenate([lower.astype(jnp.int32)] * 2, 1) == 1

    def one_slot(slot, carry):
        length = length_in[slot]
        allowed_own = (WIN * x + key < length) | (key == token)
        allowed_prev = (WIN * x - WIN + key < length) & (x > 0)
        bias = jnp.where(lower, jnp.where(allowed_own, 0.0, LOW), jnp.where(allowed_prev, 0.0, LOW))
        bias = jnp.concatenate([bias, bias], 1)

        kv_acc[...] = jnp.zeros_like(kv_acc)
        q_acc[...] = jnp.zeros_like(q_acc)
        squares = jnp.zeros((8, 128), F32)
        for k in range(tiles):
            for own in (True, False):
                core = c if own else other
                kt = tiles * core + k

                @pl.when(section > 0)
                def _():
                    def arrive(size):
                        if own:
                            pass_on(slot, k, size).wait_recv()
                            forward(slot, k, c, size).start()
                        else:
                            forward(slot, k, other, size).wait_recv()

                    sized(core, k, arrive)

                piece = h[slot, pl.ds(pl.multiple_of(TILE * kt, TILE), TILE), :]
                wide = piece.astype(F32)
                squares = squares + jnp.sum((wide * wide).reshape(TILE // 8, 8, 128), 0)
                kv_acc[...] += dot(wkv_in[kt], piece)
                if k < tiles - 1 or own:
                    q_acc[...] += dot(wq[kt], piece)
        scale = lax.rsqrt(jnp.sum(squares, 0, keepdims=True) * (1.0 / width) + EPSILON)
        cosine = cos_in[...] * scale
        sine = sin_in[...] * scale

        def rotate(first, second):
            return jnp.concatenate([first * cosine - second * sine, second * cosine + first * sine], 0)

        keys = jnp.concatenate(
            [rotate(kv_acc[64 * g : 64 * g + 32, :], kv_acc[64 * g + 32 : 64 * g + 64, :]) for g in range(2)], 0
        )
        kv_own[slot, 0] = keys.T.astype(BF16)

        @pl.when(x < chips - 1)
        def _():
            kv_copy(slot, 0).start()

        kv_own[slot, 1] = (kv_acc[128:256, :] * scale).astype(BF16)

        @pl.when(x < chips - 1)
        def _():
            kv_copy(slot, 1).start()

        q_acc[...] += dot(wq[kt], piece)
        for i in range(q.shape[0] // HEAD_DIM):
            first = q_acc[HEAD_DIM * i : HEAD_DIM * i + HALF, :]
            second = q_acc[HEAD_DIM * i + HALF : HEAD_DIM * (i + 1), :]
            q[HEAD_DIM * i : HEAD_DIM * (i + 1), :] = rotate(first, second).astype(BF16)

        cache_local(slot, 0).start()
        cache_remote(slot, 0, c).start()

        @pl.when(x > 0)
        def _():
            kv_copy(slot, 0).wait_recv()
            kv_copy(slot, 1).wait_recv()

        blank = jnp.zeros((HEAD_DIM, 256), BF16)
        ones = jnp.ones((16, 256), BF16)
        own_mask = lower_pair.astype(F32).astype(BF16)
        prev_mask = 1 - own_mask
        all_keys = jnp.concatenate([kv_own[slot, 0], kv_prev[slot, 0]], 0)
        group = shards // 2

        def raw_scores(p):
            pair = jnp.concatenate([q[128 * p : 128 * p + 64, :], q[128 * p + 64 : 128 * p + 128, :]], 1)
            return dot(all_keys, jnp.concatenate([pair, blank] if p < group else [blank, pair], 0))

        for g in range(2):
            pairs = range(group * g, group * (g + 1))
            raw = [raw_scores(p) for p in pairs]
            values = jnp.concatenate(
                [kv_own[slot, 1, 64 * g : 64 * g + 64, :], kv_prev[slot, 1, 64 * g : 64 * g + 64, :]], 1
            )
            values = jnp.concatenate([values, ones], 0)
            mixed = []
            rests = []
            for p, both in zip(pairs, raw):
                scores = jnp.where(lower_pair, both[:WIN], both[WIN:]) + bias
                sink = jnp.concatenate([sink_in[2 * p : 2 * p + 1, :], sink_in[2 * p + 1 : 2 * p + 2, :]], 1)
                top = jnp.maximum(jnp.max(scores, 0, keepdims=True), sink)
                expo = jnp.exp2(scores - top).astype(BF16)
                mixed.append(dot(values, jnp.concatenate([expo * own_mask, expo * prev_mask], 0)))
                rests.append(jnp.exp2(sink - top))
            for p, mix, rest in zip(pairs, mixed, rests):
                total = mix[HEAD_DIM : HEAD_DIM + 1, :] + rest
                context = (mix[:HEAD_DIM, :] * (1.0 / total)).astype(BF16)
                base = pl.multiple_of(128 * shards * c + 128 * p, 128)
                ctx[slot, pl.ds(base, 64), :] = context[:, :128]
                ctx[slot, pl.ds(base + 64, 64), :] = context[:, 128:]
            for m in range(group * g // 2, group * (g + 1) // 2):
                ctx_copy(slot, c, m).start()

        for k in range(tiles):
            total = jnp.zeros((TILE, 128), F32)
            for m in range(ctx_tiles):
                total = total + dot(wo[ctx_tiles * c + m, TILE * k : TILE * (k + 1), :], ctx[slot, ctx_tile(c, m), :])
            o_acc[TILE * k : TILE * (k + 1), :] = total
        for m in range(ctx_tiles):
            ctx_copy(slot, other, m).wait_recv()
        for k in range(tiles):
            total = o_acc[TILE * k : TILE * (k + 1), :]
            for m in range(ctx_tiles):
                total = total + dot(
                    wo[ctx_tiles * other + m, TILE * k : TILE * (k + 1), :], ctx[slot, ctx_tile(other, m), :]
                )
            row = pl.multiple_of(TILE * (tiles * c + k), TILE)
            h_new[slot, k] = (h[slot, pl.ds(row, TILE), :].astype(F32) + total).astype(BF16)

            @pl.when(section < sections - 1)
            def _():
                sized(c, k, lambda size: pass_on(slot, k, size).start())

        stage_v[slot] = kv_own[slot, 1].astype(F32).T.astype(BF16)
        cache_local(slot, 1).start()
        cache_remote(slot, 1, c).start()
        for k in range(tiles):
            stage_h[slot, k] = h_new[slot, k].astype(F32).T.astype(BF16)
            hid_local(slot, k).start()
            hid_remote(slot, k, c).start()
        return carry

    lax.fori_loop(0, micro, one_slot, 0)

    def finish(slot, carry):
        for k in range(tiles):
            hid_local(slot, k).wait()
            hid_remote(slot, k, other).wait_recv()
            hid_remote(slot, k, c).wait_send()

            @pl.when(section < sections - 1)
            def _():
                sized(c, k, lambda size: pass_on(slot, k, size).wait_send())

            @pl.when(section > 0)
            def _():
                sized(c, k, lambda size: forward(slot, k, c, size).wait_send())

        for which in range(2):
            cache_local(slot, which).wait()
            cache_remote(slot, which, other).wait_recv()
            cache_remote(slot, which, c).wait_send()

            @pl.when(x < chips - 1)
            def _():
                kv_copy(slot, which).wait_send()

        for m in range(ctx_tiles):
            ctx_copy(slot, c, m).wait_send()
        return carry

    lax.fori_loop(0, micro, finish, 0)
    each_step(settle)
    own_query(0, chip(1, home)).wait_send()
    own_query(1, chip(-1, home)).wait_send()
    for half in range(2):
        own_out(half, 0, chip(1, half)).wait_send()
        own_out(half, 1, chip(-1, half)).wait_send()

    @pl.when(c != home)
    def _():
        own_query(2, partner).wait_send()

    remote(wo_in.at[other], wo_slot(x, c), wo_own.at[other, 2], wo_recv.at[me], partner).wait_send()


def per_device(seqs, sections, tokens, block_order, prompt_lengths, norm_gain, w_query, w_key_value, w_out, sinks):
    micro, rows, width = tokens.shape
    padded = -(-width // (2 * TILE)) * 2 * TILE
    tiles = padded // (2 * TILE)
    shards = seqs // 2
    me = lax.axis_index("seq")
    core = me % 2
    extra = padded - width
    gain = norm_gain[0][:, None]
    kv_width = w_key_value.shape[2] // 2

    def turned(weight):
        weight = jnp.pad(weight.astype(BF16), ((0, extra), (0, 0)))
        return weight.reshape(padded // TILE, TILE, weight.shape[1]).transpose(0, 2, 1)

    wq = turned(w_query[0].astype(F32) * (gain * (HEAD_DIM**-0.5 * LOG2E)))
    pair = jnp.concatenate(
        [
            lax.dynamic_slice_in_dim(w_key_value[0], core * (kv_width // 2), kv_width // 2, 1),
            lax.dynamic_slice_in_dim(w_key_value[0], kv_width + core * (kv_width // 2), kv_width // 2, 1),
        ],
        1,
    )
    wkv = turned(pair.astype(F32) * gain)
    wo = jnp.pad(w_out[0], ((0, 0), (0, extra))).reshape(w_out.shape[1], 2, padded // 2).transpose(1, 2, 0)
    tok = jnp.pad(tokens[block_order], ((0, 0), (0, 0), (0, extra)))
    lengths = prompt_lengths[block_order]
    freq = jnp.exp(jnp.arange(HALF, dtype=F32) * (-2.0 * math.log(THETA) / HEAD_DIM))
    positions = (me // 2) * (2 * rows) + jnp.arange(2 * rows, dtype=jnp.int32)
    angles = freq[:, None] * positions.astype(F32)[None, :]
    heads = 2 * shards
    sink = lax.dynamic_slice_in_dim(sinks[0], core * heads, heads, 0)
    sink = jnp.broadcast_to(sink[:, None] * LOG2E, (heads, 128))

    vmem = pl.BlockSpec(memory_space=pltpu.VMEM)
    dma = pltpu.SemaphoreType.DMA
    cells = 64 * heads
    hidden, cache = pl.pallas_call(
        functools.partial(kernel, seqs, sections, micro, width),
        out_shape=(
            jax.ShapeDtypeStruct((micro, rows, padded), BF16),
            jax.ShapeDtypeStruct((micro, rows, 2 * kv_width), BF16),
        ),
        in_specs=[vmem] * 7 + [pl.BlockSpec(memory_space=pltpu.SMEM)],
        out_specs=(pl.BlockSpec(memory_space=pl.ANY), pl.BlockSpec(memory_space=pl.ANY)),
        scratch_shapes=[
            pltpu.VMEM((2 * tiles, cells, TILE), BF16),
            pltpu.VMEM((shards, tiles * TILE, TILE), BF16),
            pltpu.VMEM((micro, padded, 128), BF16),
            pltpu.VMEM((micro, 128, padded), BF16),
            pltpu.VMEM((256, 128), F32),
            pltpu.VMEM((cells, 128), F32),
            pltpu.VMEM((cells, 128), BF16),
            pltpu.VMEM((micro, 2, 128, 128), BF16),
            pltpu.VMEM((micro, 2, 128, 128), BF16),
            pltpu.VMEM((micro, 2 * cells, 128), BF16),
            pltpu.VMEM((tiles * TILE, 128), F32),
            pltpu.VMEM((micro, tiles, TILE, 128), BF16),
            pltpu.VMEM((micro, tiles, 128, TILE), BF16),
            pltpu.VMEM((micro, 128, 128), BF16),
            dma((shards,)), dma((3,)), dma((shards,)),
            dma((seqs,)), dma((2, 3)), dma((seqs,)),
            dma, dma((2,)),
            dma((micro, tiles)), dma((micro, tiles)),
            dma((micro, tiles)), dma((micro, tiles)),
            dma((micro, 2)), dma((micro, 2)),
            dma((micro, shards // 2)), dma((micro, shards // 2)),
            dma((micro, tiles)), dma((micro, tiles)), dma((micro, tiles)),
            dma((micro, 2)), dma((micro, 2)), dma((micro, 2)),
        ],
        compiler_params=pltpu.CompilerParams(
            collective_id=0, has_side_effects=True, vmem_limit_bytes=50 * 1024 * 1024
        ),
    )(wq, wkv, wo, tok, jnp.cos(angles), jnp.sin(angles), sink, lengths)
    return hidden[None, :, :, :width], cache[None]


def solution(mesh):
    in_specs = (
        P("groups", "seq", None),
        P("groups"),
        P("groups"),
        P("section", None),
        P("section", None, "seq"),
        P("section", None, None),
        P("section", "seq", None),
        P("section", None),
    )
    out_specs = (P("section", "groups", "seq", None), P("section", "groups", "seq", None))
    body = functools.partial(per_device, mesh.shape["seq"], mesh.shape["section"])
    return jax.shard_map(body, mesh=mesh, in_specs=in_specs, out_specs=out_specs, check_vma=False)
```

```python
import functools
import math

import jax
import jax.numpy as jnp
from jax import lax
from jax.experimental import pallas as pl
from jax.experimental.pallas import tpu as pltpu
from jax.sharding import PartitionSpec as P

MESH = pl.DeviceIdType.MESH
HEAD_DIM = 64
HALF = HEAD_DIM // 2
WIN = 128
TILE = 256
THETA = 150000.0
EPSILON = 1e-05
LOW = -1e30
LOG2E = math.log2(math.e)
F32 = jnp.float32
BF16 = jnp.bfloat16


def dot(a, b):
    return jnp.dot(a, b, preferred_element_type=F32)


def kernel(
    seqs, sections, micro, width,
    wq_in, wkv_in, wo_in, tok_in, cos_in, sin_in, sink_in, length_in, order_in,
    hid_out, cache_out,
    wq, wo, h, tok, kv_acc, q_acc, q, kv_own, kv_prev, ctx, o_acc, h_new, stage_h, stage_v, aq, ao,
    wq_recv, wq_own, wq_relay, wo_recv, wo_own, wo_relay,
    aq_recv, aq_relay, aq_up, ao_recv, ao_relay, ao_up,
    tok_send, tok_recv, h_send, h_recv, f_send, f_recv, kv_send, kv_recv, c_send, c_recv,
    oh_local, oh_send, oh_recv, oc_local, oc_send, oc_recv,
):
    chips = seqs // 2
    half_chips = chips // 2
    shards = seqs // 2
    tiles = h.shape[1] // (2 * TILE)
    cut = TILE * tiles - ao.shape[1]
    ctx_tiles = shards // 2
    me = lax.axis_index("seq")
    section = lax.axis_index("section")
    x = me // 2
    c = me % 2
    other = 1 - c
    partner = {"seq": 2 * x + other}

    def chip(step, core):
        return {"seq": 2 * ((x + step + chips) % chips) + core}

    def remote(src, dst, send, recv, target):
        return pltpu.make_async_remote_copy(
            src_ref=src, dst_ref=dst, send_sem=send, recv_sem=recv, device_id=target, device_id_type=MESH
        )

    first = section == 0
    last = section == sections - 1
    above = (section + 1) % sections
    below = (section + sections - 1) % sections
    up = {"section": above}
    barrier = pltpu.get_barrier_semaphore()
    greeted = [partner] + [chip(step, core) for step in (1, -1) for core in range(2)]
    greeted += [{"section": level, "seq": 2 * x + core} for level in (above, below) for core in range(2)]
    for target in greeted:
        pl.semaphore_signal(barrier, inc=1, device_id=target, device_id_type=MESH)
    pl.semaphore_wait(barrier, len(greeted))

    home = x // half_chips
    query_cuts = (0, tiles, 2 * tiles - 1, 2 * tiles)
    out_cuts = (0, cut, TILE * tiles)
    dead = h.shape[1] - width
    query_pieces, out_pieces = range(3), range(2)
    query_tail, out_tail = 2, 1

    def query_slot(index, piece):
        lo, hi = query_cuts[piece : piece + 2]
        return wq.at[lo:hi, pl.ds(pl.multiple_of(128 * index, 128), 128), :]

    def out_slot(owner, core, piece):
        lo, hi = out_cuts[piece : piece + 2]
        return wo.at[owner, lo:hi, pl.ds(pl.multiple_of(128 * core, 128), 128)]

    def query_source(piece):
        return wq_in.at[query_cuts[piece] : query_cuts[piece + 1]]

    def out_source(half, piece):
        return wo_in.at[half, out_cuts[piece] : out_cuts[piece + 1], :]

    def aid_query(index):
        return aq.at[:, pl.ds(pl.multiple_of(128 * index, 128), 128), :]

    def aid_out(owner, core, size):
        return ao.at[owner, :size, pl.ds(pl.multiple_of(128 * core, 128), 128)]

    def halves(half, act):
        if isinstance(half, int):
            act(TILE * tiles - cut - (dead if half else 0))
        else:
            for each in range(2):

                @pl.when(half == each)
                def _():
                    act(TILE * tiles - cut - (dead if each else 0))

    mine = me - shards * home

    def own_query(piece, which, target):
        return remote(
            query_source(piece), query_slot(mine, piece), wq_own.at[piece, which], wq_recv.at[piece, mine], target
        )

    def local_query(piece, index):
        return pltpu.make_async_copy(query_source(piece), query_slot(index, piece), wq_recv.at[piece, index])

    def own_out(half, piece, which, target):
        return remote(
            out_source(half, piece), out_slot(x, c, piece), wo_own.at[half, piece, which], wo_recv.at[piece, me], target
        )

    def local_out(piece, core):
        return pltpu.make_async_copy(out_source(c, piece), out_slot(x, core, piece), wo_recv.at[piece, 2 * x + core])

    def lend_query():
        target = {"section": below, "seq": 2 * x + home}
        return remote(query_source(query_tail), aid_query(mine), wq_own.at[query_tail, 0], aq_recv.at[mine], target)

    def lend_out(half, size):
        target = {"section": below, "seq": 2 * x + half}
        source = wo_in.at[half, cut : cut + size, :]
        return remote(source, aid_out(x, c, size), wo_own.at[half, out_tail, 0], ao_recv.at[me], target)

    def own_queries(act):
        for piece in query_pieces:

            def ring():
                act(own_query(piece, 0, chip(1, home)))
                act(own_query(piece, 1, chip(-1, home)))

            if piece == query_tail:
                pl.when(~first)(ring)
                pl.when(first)(lambda: act(lend_query()))
            else:
                ring()

            @pl.when(c != home)
            def _():
                act(own_query(piece, 2, partner))

    def own_outs(act):
        for piece in out_pieces:
            for half in range(2):

                def ring():
                    act(own_out(half, piece, 0, chip(1, half)))
                    act(own_out(half, piece, 1, chip(-1, half)))

                if piece == out_tail:
                    pl.when(~first)(ring)
                else:
                    ring()
            act(own_out(other, piece, 2, partner))

    def lend_outs(act):
        @pl.when(first)
        def _():
            for half in range(2):
                halves(half, lambda size: act(lend_out(half, size)))

    def query_copy(index, sign, piece):
        slot = query_slot(index, piece)
        return remote(slot, slot, wq_relay.at[piece, index], wq_recv.at[piece, index], chip(sign, c))

    def out_copy(owner, core, sign, piece):
        slot = out_slot(owner, core, piece)
        index = 2 * owner + core
        return remote(slot, slot, wo_relay.at[piece, index], wo_recv.at[piece, index], chip(sign, c))

    def owner_of(step, sign):
        return (x - sign * step + chips) % chips

    query_hops = {1: half_chips, -1: half_chips - 1}
    out_hops = {1: half_chips - 1, -1: half_chips}

    def each_query(step, sign, act):
        owner = owner_of(step, sign)
        held = owner // half_chips == c
        for piece in query_pieces:

            @pl.when(held & ~first if piece == query_tail else held)
            def _():
                for core in range(2):
                    index = 2 * owner + core - shards * c
                    act(lambda: query_copy(index, sign, piece), step < query_hops[sign])

    def each_out(step, sign, act):
        owner = owner_of(step, sign)
        for piece in out_pieces:

            def held():
                for core in range(2):
                    act(lambda: out_copy(owner, core, sign, piece), step < out_hops[sign])

            if piece == out_tail:
                pl.when(~first)(held)
            else:
                held()

    arrivals = []
    for sign in (1, -1):
        line = [(each_query, step) for step in range(1, half_chips)] + [(each_out, 1)]
        line += [(each_query, step) for step in range(half_chips, query_hops[sign] + 1)]
        line += [(each_out, step) for step in range(2, out_hops[sign] + 1)]
        time = 0
        for kind, step in line:
            time += 5 if kind is each_query else 3
            arrivals.append((time, sign, kind, step))
    arrivals.sort(key=lambda arrival: (arrival[0], -arrival[1]))
    needed = [a for a in range(len(arrivals)) if arrivals[a][2] is each_query][-1] + 1
    ending = max(needed, len(arrivals) - 2)

    def take(low, high, act):
        for _, sign, kind, step in arrivals[low:high]:
            kind(step, sign, act)

    def relay(make, more):
        copy = make()
        copy.wait_recv()
        if more:
            copy.start()

    def settle(make, more):
        if more:
            make().wait_send()

    def steps(low, high, each, act):
        def body(step, carry):
            each(step, act)
            return carry

        lax.fori_loop(low, high, body, 0)

    def aid_query_copy(index, sign):
        slot = aid_query(index)
        return remote(slot, slot, aq_relay.at[(1 - sign) // 2, index], aq_recv.at[index], chip(sign, c))

    def aid_query_up(index):
        return remote(
            aid_query(index), query_slot(index, query_tail), aq_up.at[index], wq_recv.at[query_tail, index], up
        )

    def aid_out_copy(owner, core, sign, size):
        slot = aid_out(owner, core, size)
        index = 2 * owner + core
        return remote(slot, slot, ao_relay.at[(1 - sign) // 2, index], ao_recv.at[index], chip(sign, c))

    def aid_out_up(owner, core, size):
        index = 2 * owner + core
        target = wo.at[owner, cut : cut + size, pl.ds(pl.multiple_of(128 * core, 128), 128)]
        return remote(aid_out(owner, core, size), target, ao_up.at[index], wo_recv.at[out_tail, index], up)

    def aid_own_query(act):
        @pl.when(c == home)
        def _():
            for core in range(2):
                index = 2 * x + core - shards * c
                act(aid_query_copy(index, 1), aid_query_copy(index, -1))

    def aid_own_out(act):
        def both(size):
            for core in range(2):
                act(aid_out_copy(x, core, 1, size), aid_out_copy(x, core, -1, size))

        halves(c, both)

    def aid_each_query(step, act):
        for sign in (1, -1):
            owner = owner_of(step, sign)

            @pl.when((step <= query_hops[sign]) & (owner // half_chips == c))
            def _():
                for core in range(2):
                    index = 2 * owner + core - shards * c
                    act(aid_query_copy(index, sign), aid_query_up(index), step < query_hops[sign])

    def aid_each_out(step, act):
        for sign in (-1, 1):
            owner = owner_of(step, sign)

            @pl.when(step <= out_hops[sign])
            def _():
                def both(size):
                    for core in range(2):
                        act(
                            aid_out_copy(owner, core, sign, size), aid_out_up(owner, core, size),
                            step < out_hops[sign],
                        )

                halves(c, both)

    def aid_send(right, left):
        right.wait_recv()
        right.start()
        left.start()

    def aid_sent(right, left):
        right.wait_send()
        left.wait_send()

    def aid_relay(along, upward, more):
        along.wait_recv()
        upward.start()

        @pl.when(more)
        def _():
            along.start()

    def aid_settle(along, upward, more):
        upward.wait_send()

        @pl.when(more)
        def _():
            along.wait_send()

    def start(copy):
        copy.start()

    def sent(copy):
        copy.wait_send()

    @pl.when(last)
    def _():
        aid_own_query(aid_send)
        aid_own_out(aid_send)
        steps(1, half_chips + 1, aid_each_query, aid_relay)
        steps(1, half_chips + 1, aid_each_out, aid_relay)

    own_queries(start)
    lend_outs(start)
    for piece in query_pieces:

        @pl.when(c == home)
        def _():
            local_query(piece, mine).start()

    for piece in out_pieces:
        local_out(piece, c).start()

    rows = pl.ds(pl.multiple_of(64 * c, 64), 64)
    other_rows = pl.ds(pl.multiple_of(64 * other, 64), 64)

    def tok_remote():
        return remote(tok_in, tok.at[:, rows, :], tok_send, tok_recv.at[1], partner)

    def tok_local():
        return pltpu.make_async_copy(tok_in, tok.at[:, rows, :], tok_recv.at[0])

    h[:, width:, :] = jnp.zeros((micro, h.shape[1] - width, 128), BF16)

    @pl.when(first & (c == 1))
    def _():
        for step in range(1, chips):
            wo[(x + step) % chips, TILE * tiles - dead :, :] = jnp.zeros((dead, TILE), BF16)

    @pl.when(x == 0)
    def _():
        kv_prev[...] = jnp.zeros_like(kv_prev)

    @pl.when(first)
    def _():
        tok_remote().start()
        tok_local().start()
        tok_local().wait()
        tok_remote().wait()

        def turn(slot, carry):
            block = order_in[slot]
            for low in range(0, width, 128):
                high = min(low + 128, width)
                h[slot, low:high, :] = tok[block, :, low:high].astype(F32).T.astype(BF16)
            return carry

        lax.fori_loop(0, micro, turn, 0)

    before = 2 * (half_chips - 2)
    take(0, before, relay)
    own_outs(start)
    take(before, needed, relay)

    @pl.when(c == home)
    def _():
        for piece in query_pieces:
            for core in range(2):
                local_query(piece, 2 * x + core - shards * c).wait()

    @pl.when(first)
    def _():
        def body(step, carry):
            for sign in (1, -1):
                owner = owner_of(step, sign)

                @pl.when((step <= query_hops[sign]) & (owner // half_chips == c))
                def _():
                    for core in range(2):
                        query_copy(2 * owner + core - shards * c, sign, query_tail).wait_recv()

            return carry

        lax.fori_loop(1, half_chips + 1, body, 0)

    def finish_outs():
        for piece in out_pieces:
            for core in range(2):
                local_out(piece, core).wait()

        @pl.when(first)
        def _():
            def body(step, carry):
                for sign in (-1, 1):
                    owner = owner_of(step, sign)

                    @pl.when(step <= out_hops[sign])
                    def _():
                        def both(size):
                            for core in range(2):
                                aid_out_up(owner, core, size).wait_recv()

                        halves(c, both)

                return carry

            lax.fori_loop(1, half_chips + 1, body, 0)

    short = width - (2 * tiles - 1) * TILE

    def sized(core, k, act):
        if k < tiles - 1 or short == TILE:
            act(TILE)
        else:

            @pl.when(core == 0)
            def _():
                act(TILE)

            @pl.when(core == 1)
            def _():
                act(short)

    def h_tile(slot, k, size):
        return h.at[slot, pl.ds(pl.multiple_of(TILE * k, TILE), size), :]

    def pass_on(slot, k, size):
        return remote(
            h_new.at[slot, k, :size, :], h_tile(slot, tiles * c + k, size), h_send.at[slot, k], h_recv.at[slot, k], up
        )

    def forward(slot, k, core, size):
        piece = h_tile(slot, tiles * core + k, size)
        return remote(piece, piece, f_send.at[slot, k], f_recv.at[slot, k], partner)

    def kv_copy(slot, which):
        return remote(
            kv_own.at[slot, which], kv_prev.at[slot, which], kv_send.at[slot, which], kv_recv.at[slot, which],
            chip(1, c),
        )

    def ctx_tile(core, m):
        return pl.ds(pl.multiple_of(TILE * (ctx_tiles * core + m), TILE), TILE)

    def ctx_copy(slot, core, m):
        piece = ctx.at[slot, ctx_tile(core, m), :]
        return remote(piece, piece, c_send.at[slot, m], c_recv.at[slot, m], partner)

    def hid_columns(core, k):
        return pl.ds(pl.multiple_of(TILE * (tiles * core + k), TILE), TILE)

    def hid_local(slot, k):
        return pltpu.make_async_copy(
            stage_h.at[slot, k, rows, :], hid_out.at[slot, :, hid_columns(c, k)], oh_local.at[slot, k]
        )

    def hid_remote(slot, k, core):
        return remote(
            stage_h.at[slot, k, other_rows, :], hid_out.at[slot, :, hid_columns(core, k)],
            oh_send.at[slot, k], oh_recv.at[slot, k], partner,
        )

    def cache_columns(core, which):
        return pl.ds(pl.multiple_of(256 * which + 128 * core, 128), 128)

    def cache_source(slot, which, span):
        return kv_own.at[slot, 0, span, :] if which == 0 else stage_v.at[slot, span, :]

    def cache_local(slot, which):
        return pltpu.make_async_copy(
            cache_source(slot, which, rows), cache_out.at[slot, :, cache_columns(c, which)], oc_local.at[slot, which]
        )

    def cache_remote(slot, which, core):
        return remote(
            cache_source(slot, which, other_rows), cache_out.at[slot, :, cache_columns(core, which)],
            oc_send.at[slot, which], oc_recv.at[slot, which], partner,
        )

    key = lax.broadcasted_iota(jnp.int32, (WIN, 128), 0)
    token = lax.broadcasted_iota(jnp.int32, (WIN, 128), 1)
    lower = key <= token
    lower_pair = jnp.concatenate([lower.astype(jnp.int32)] * 2, 1) == 1

    def project(slot):
        kv_acc[...] = jnp.zeros_like(kv_acc)
        q_acc[...] = jnp.zeros_like(q_acc)
        squares = jnp.zeros((8, 128), F32)
        for own in (True, False):
            for k in range(tiles):
                core = c if own else other
                kt = tiles * core + k

                @pl.when(section > 0)
                def _():
                    def arrive(size):
                        if own:
                            pass_on(slot, k, size).wait_recv()
                            forward(slot, k, c, size).start()
                        else:
                            forward(slot, k, other, size).wait_recv()

                    sized(core, k, arrive)

                piece = h[slot, pl.ds(pl.multiple_of(TILE * kt, TILE), TILE), :]
                wide = piece.astype(F32)
                squares = squares + jnp.sum((wide * wide).reshape(TILE // 8, 8, 128), 0)
                kv_acc[...] += dot(wkv_in[kt], piece)
                if k < tiles - 1 or own:
                    q_acc[...] += dot(wq[kt], piece)
        scale = lax.rsqrt(jnp.sum(squares, 0, keepdims=True) * (1.0 / width) + EPSILON)
        cosine = cos_in[...] * scale
        sine = sin_in[...] * scale

        def rotate(first, second):
            return jnp.concatenate([first * cosine - second * sine, second * cosine + first * sine], 0)

        keys = jnp.concatenate(
            [rotate(kv_acc[64 * g : 64 * g + 32, :], kv_acc[64 * g + 32 : 64 * g + 64, :]) for g in range(2)], 0
        )
        kv_own[slot, 0] = keys.T.astype(BF16)

        @pl.when(x < chips - 1)
        def _():
            kv_copy(slot, 0).start()

        kv_own[slot, 1] = (kv_acc[128:256, :] * scale).astype(BF16)

        @pl.when(x < chips - 1)
        def _():
            kv_copy(slot, 1).start()

        q_acc[...] += dot(wq[kt], piece)
        for i in range(q.shape[0] // HEAD_DIM):
            first = q_acc[HEAD_DIM * i : HEAD_DIM * i + HALF, :]
            second = q_acc[HEAD_DIM * i + HALF : HEAD_DIM * (i + 1), :]
            q[HEAD_DIM * i : HEAD_DIM * (i + 1), :] = rotate(first, second).astype(BF16)

    def attend(slot):
        length = length_in[order_in[slot]]
        allowed_own = (WIN * x + key < length) | (key == token)
        allowed_prev = (WIN * x - WIN + key < length) & (x > 0)
        bias = jnp.where(lower, jnp.where(allowed_own, 0.0, LOW), jnp.where(allowed_prev, 0.0, LOW))
        bias = jnp.concatenate([bias, bias], 1)

        @pl.when(x > 0)
        def _():
            kv_copy(slot, 0).wait_recv()
            kv_copy(slot, 1).wait_recv()

        blank = jnp.zeros((HEAD_DIM, 256), BF16)
        ones = jnp.ones((16, 256), BF16)
        own_mask = lower_pair.astype(F32).astype(BF16)
        prev_mask = 1 - own_mask
        all_keys = jnp.concatenate([kv_own[slot, 0], kv_prev[slot, 0]], 0)
        group = shards // 2

        def raw_scores(p):
            pair = jnp.concatenate([q[128 * p : 128 * p + 64, :], q[128 * p + 64 : 128 * p + 128, :]], 1)
            return dot(all_keys, jnp.concatenate([pair, blank] if p < group else [blank, pair], 0))

        for g in range(2):
            pairs = range(group * g, group * (g + 1))
            raw = [raw_scores(p) for p in pairs]
            values = jnp.concatenate(
                [kv_own[slot, 1, 64 * g : 64 * g + 64, :], kv_prev[slot, 1, 64 * g : 64 * g + 64, :]], 1
            )
            values = jnp.concatenate([values, ones], 0)
            mixed = []
            rests = []
            for p, both in zip(pairs, raw):
                scores = jnp.where(lower_pair, both[:WIN], both[WIN:]) + bias
                sink = jnp.concatenate([sink_in[2 * p : 2 * p + 1, :], sink_in[2 * p + 1 : 2 * p + 2, :]], 1)
                top = jnp.maximum(jnp.max(scores, 0, keepdims=True), sink)
                expo = jnp.exp2(scores - top).astype(BF16)
                mixed.append(dot(values, jnp.concatenate([expo * own_mask, expo * prev_mask], 0)))
                rests.append(jnp.exp2(sink - top))
            for p, mix, rest in zip(pairs, mixed, rests):
                total = mix[HEAD_DIM : HEAD_DIM + 1, :] + rest
                context = (mix[:HEAD_DIM, :] * (1.0 / total)).astype(BF16)
                base = pl.multiple_of(128 * shards * c + 128 * p, 128)
                ctx[slot, pl.ds(base, 64), :] = context[:, :128]
                ctx[slot, pl.ds(base + 64, 64), :] = context[:, 128:]
            for m in range(group * g // 2, group * (g + 1) // 2):
                ctx_copy(slot, c, m).start()

    def emit(slot):
        def part(core, k, m):
            return dot(wo[ctx_tiles * core + m, TILE * k : TILE * (k + 1), :], ctx[slot, ctx_tile(core, m), :])

        early, late = range(ctx_tiles // 2), range(ctx_tiles // 2, ctx_tiles)
        for m in early:
            ctx_copy(slot, other, m).wait_recv()
        for k in range(tiles):
            total = part(c, k, 0)
            for m in range(1, ctx_tiles):
                total = total + part(c, k, m)
            for m in early:
                total = total + part(other, k, m)
            o_acc[TILE * k : TILE * (k + 1), :] = total
        for m in late:
            ctx_copy(slot, other, m).wait_recv()
        for k in range(tiles):
            total = o_acc[TILE * k : TILE * (k + 1), :]
            for m in late:
                total = total + part(other, k, m)
            row = pl.multiple_of(TILE * (tiles * c + k), TILE)
            h_new[slot, k] = (h[slot, pl.ds(row, TILE), :].astype(F32) + total).astype(BF16)

            @pl.when(section < sections - 1)
            def _():
                sized(c, k, lambda size: pass_on(slot, k, size).start())

        cache_local(slot, 0).start()
        cache_remote(slot, 0, c).start()
        stage_v[slot] = kv_own[slot, 1].astype(F32).T.astype(BF16)
        cache_local(slot, 1).start()
        cache_remote(slot, 1, c).start()
        for k in range(tiles):
            stage_h[slot, k] = h_new[slot, k].astype(F32).T.astype(BF16)
            hid_local(slot, k).start()
            hid_remote(slot, k, c).start()

    @pl.when(first)
    def _():
        project(0)

    take(needed, ending, relay)

    @pl.when(~first)
    def _():
        project(0)

    attend(0)

    @pl.when(first)
    def _():
        project(1)

    take(ending, len(arrivals), relay)
    finish_outs()

    def one_slot(slot, carry):
        emit(slot)

        @pl.when(~first & (slot < micro - 1))
        def _():
            project(slot + 1)

        @pl.when(slot < micro - 1)
        def _():
            attend(slot + 1)

        @pl.when(first & (slot < micro - 2))
        def _():
            project(slot + 2)

        return carry

    lax.fori_loop(0, micro, one_slot, 0)

    def finish(slot, carry):
        for k in range(tiles):
            hid_local(slot, k).wait()
            hid_remote(slot, k, other).wait_recv()
            hid_remote(slot, k, c).wait_send()

            @pl.when(section < sections - 1)
            def _():
                sized(c, k, lambda size: pass_on(slot, k, size).wait_send())

            @pl.when(section > 0)
            def _():
                sized(c, k, lambda size: forward(slot, k, c, size).wait_send())

        for which in range(2):
            cache_local(slot, which).wait()
            cache_remote(slot, which, other).wait_recv()
            cache_remote(slot, which, c).wait_send()

            @pl.when(x < chips - 1)
            def _():
                kv_copy(slot, which).wait_send()

        for m in range(ctx_tiles):
            ctx_copy(slot, c, m).wait_send()
        return carry

    lax.fori_loop(0, micro, finish, 0)
    take(0, len(arrivals), settle)
    own_queries(sent)
    own_outs(sent)
    lend_outs(sent)

    @pl.when(last)
    def _():
        aid_own_query(aid_sent)
        aid_own_out(aid_sent)
        steps(1, half_chips + 1, aid_each_query, aid_settle)
        steps(1, half_chips + 1, aid_each_out, aid_settle)


def per_device(seqs, sections, tokens, block_order, prompt_lengths, norm_gain, w_query, w_key_value, w_out, sinks):
    micro, rows, width = tokens.shape
    padded = -(-width // (2 * TILE)) * 2 * TILE
    tiles = padded // (2 * TILE)
    shards = seqs // 2
    me = lax.axis_index("seq")
    core = me % 2
    extra = padded - width
    gain = norm_gain[0][:, None]
    kv_width = w_key_value.shape[2] // 2

    def turned(weight):
        weight = jnp.pad(weight.astype(BF16), ((0, extra), (0, 0)))
        return weight.reshape(padded // TILE, TILE, weight.shape[1]).transpose(0, 2, 1)

    wq = turned(w_query[0].astype(F32) * (gain * (HEAD_DIM**-0.5 * LOG2E)))
    pair = jnp.concatenate(
        [
            lax.dynamic_slice_in_dim(w_key_value[0], core * (kv_width // 2), kv_width // 2, 1),
            lax.dynamic_slice_in_dim(w_key_value[0], kv_width + core * (kv_width // 2), kv_width // 2, 1),
        ],
        1,
    )
    wkv = turned(pair.astype(F32) * gain)
    wo = jnp.pad(w_out[0], ((0, 0), (0, extra))).reshape(w_out.shape[1], 2, padded // 2).transpose(1, 2, 0)
    freq = jnp.exp(jnp.arange(HALF, dtype=F32) * (-2.0 * math.log(THETA) / HEAD_DIM))
    positions = (me // 2) * (2 * rows) + jnp.arange(2 * rows, dtype=jnp.int32)
    angles = freq[:, None] * positions.astype(F32)[None, :]
    heads = 2 * shards
    sink = lax.dynamic_slice_in_dim(sinks[0], core * heads, heads, 0)
    sink = jnp.broadcast_to(sink[:, None] * LOG2E, (heads, 128))

    vmem = pl.BlockSpec(memory_space=pltpu.VMEM)
    dma = pltpu.SemaphoreType.DMA
    cells = 64 * heads
    hidden, cache = pl.pallas_call(
        functools.partial(kernel, seqs, sections, micro, width),
        out_shape=(
            jax.ShapeDtypeStruct((micro, rows, padded), BF16),
            jax.ShapeDtypeStruct((micro, rows, 2 * kv_width), BF16),
        ),
        in_specs=[vmem] * 7 + [pl.BlockSpec(memory_space=pltpu.SMEM)] * 2,
        out_specs=(pl.BlockSpec(memory_space=pl.ANY), pl.BlockSpec(memory_space=pl.ANY)),
        scratch_shapes=[
            pltpu.VMEM((2 * tiles, cells, TILE), BF16),
            pltpu.VMEM((shards, tiles * TILE, TILE), BF16),
            pltpu.VMEM((micro, padded, 128), BF16),
            pltpu.VMEM((micro, 128, width), BF16),
            pltpu.VMEM((256, 128), F32),
            pltpu.VMEM((cells, 128), F32),
            pltpu.VMEM((cells, 128), BF16),
            pltpu.VMEM((micro, 2, 128, 128), BF16),
            pltpu.VMEM((micro, 2, 128, 128), BF16),
            pltpu.VMEM((micro, 2 * cells, 128), BF16),
            pltpu.VMEM((tiles * TILE, 128), F32),
            pltpu.VMEM((micro, tiles, TILE, 128), BF16),
            pltpu.VMEM((micro, tiles, 128, TILE), BF16),
            pltpu.VMEM((micro, 128, 128), BF16),
            pltpu.VMEM((1, cells, TILE), BF16),
            pltpu.VMEM((shards, TILE * tiles // 2, TILE), BF16),
            dma((3, shards)), dma((3, 3)), dma((3, shards)),
            dma((2, seqs)), dma((2, 2, 3)), dma((2, seqs)),
            dma((shards,)), dma((2, shards)), dma((shards,)),
            dma((seqs,)), dma((2, seqs)), dma((seqs,)),
            dma, dma((2,)),
            dma((micro, tiles)), dma((micro, tiles)),
            dma((micro, tiles)), dma((micro, tiles)),
            dma((micro, 2)), dma((micro, 2)),
            dma((micro, shards // 2)), dma((micro, shards // 2)),
            dma((micro, tiles)), dma((micro, tiles)), dma((micro, tiles)),
            dma((micro, 2)), dma((micro, 2)), dma((micro, 2)),
        ],
        compiler_params=pltpu.CompilerParams(
            collective_id=0, has_side_effects=True, vmem_limit_bytes=50 * 1024 * 1024
        ),
    )(wq, wkv, wo, tokens, jnp.cos(angles), jnp.sin(angles), sink, prompt_lengths, block_order)
    return hidden[None, :, :, :width], cache[None]


def solution(mesh):
    in_specs = (
        P("groups", "seq", None),
        P("groups"),
        P("groups"),
        P("section", None),
        P("section", None, "seq"),
        P("section", None, None),
        P("section", "seq", None),
        P("section", None),
    )
    out_specs = (P("section", "groups", "seq", None), P("section", "groups", "seq", None))
    body = functools.partial(per_device, mesh.shape["seq"], mesh.shape["section"])
    return jax.shard_map(body, mesh=mesh, in_specs=in_specs, out_specs=out_specs, check_vma=False)
```

```python
import functools
import math

import jax
import jax.numpy as jnp
from jax import lax
from jax.experimental import pallas as pl
from jax.experimental.pallas import tpu as pltpu
from jax.sharding import PartitionSpec as P

MESH = pl.DeviceIdType.MESH
HEAD_DIM = 64
HALF = HEAD_DIM // 2
WIN = 128
TILE = 256
THETA = 150000.0
EPSILON = 1e-05
LOW = -1e30
LOG2E = math.log2(math.e)
F32 = jnp.float32
BF16 = jnp.bfloat16


def dot(a, b):
    return jnp.dot(a, b, preferred_element_type=F32)


def kernel(
    seqs, sections, micro, width,
    wq_in, wkv_in, wo_in, tok_in, cos_in, sin_in, sink_in, length_in, order_in,
    hid_out, cache_out,
    wq, wo, h, tok, kv_acc, q_acc, q, kv_own, kv_prev, ctx, o_acc, h_new, stage_h, stage_v, aq, ao,
    wq_recv, wq_own, wq_relay, wo_recv, wo_own, wo_relay,
    aq_recv, aq_relay, aq_up, ao_recv, ao_relay, ao_up,
    tok_send, tok_recv, h_send, h_recv, f_send, f_recv, kv_send, kv_recv, c_send, c_recv,
    oh_local, oh_send, oh_recv, oc_local, oc_send, oc_recv,
):
    chips = seqs // 2
    half_chips = chips // 2
    shards = seqs // 2
    tiles = h.shape[1] // (2 * TILE)
    cut = TILE * tiles - ao.shape[1]
    ctx_tiles = shards // 2
    me = lax.axis_index("seq")
    section = lax.axis_index("section")
    x = me // 2
    c = me % 2
    other = 1 - c
    partner = {"seq": 2 * x + other}

    def chip(step, core):
        return {"seq": 2 * ((x + step + chips) % chips) + core}

    def remote(src, dst, send, recv, target):
        return pltpu.make_async_remote_copy(
            src_ref=src, dst_ref=dst, send_sem=send, recv_sem=recv, device_id=target, device_id_type=MESH
        )

    first = section == 0
    last = section == sections - 1
    above = (section + 1) % sections
    below = (section + sections - 1) % sections
    up = {"section": above}
    barrier = pltpu.get_barrier_semaphore()
    greeted = [partner] + [chip(step, core) for step in (1, -1) for core in range(2)]
    greeted += [{"section": level, "seq": 2 * x + core} for level in (above, below) for core in range(2)]
    for target in greeted:
        pl.semaphore_signal(barrier, inc=1, device_id=target, device_id_type=MESH)
    pl.semaphore_wait(barrier, len(greeted))

    home = x // half_chips
    query_cuts = (0, tiles, 2 * tiles - 1, 2 * tiles)
    out_cuts = (0, cut, TILE * tiles)
    dead = h.shape[1] - width
    query_pieces, out_pieces = range(3), range(2)
    query_tail, out_tail = 2, 1

    def query_slot(index, piece):
        lo, hi = query_cuts[piece : piece + 2]
        return wq.at[lo:hi, pl.ds(pl.multiple_of(128 * index, 128), 128), :]

    def out_slot(owner, core, piece):
        lo, hi = out_cuts[piece : piece + 2]
        return wo.at[owner, lo:hi, pl.ds(pl.multiple_of(128 * core, 128), 128)]

    def query_source(piece):
        return wq_in.at[query_cuts[piece] : query_cuts[piece + 1]]

    def out_source(half, piece):
        return wo_in.at[half, out_cuts[piece] : out_cuts[piece + 1], :]

    def aid_query(index):
        return aq.at[:, pl.ds(pl.multiple_of(128 * index, 128), 128), :]

    def aid_out(owner, core, size):
        return ao.at[owner, :size, pl.ds(pl.multiple_of(128 * core, 128), 128)]

    def halves(half, act):
        if isinstance(half, int):
            act(TILE * tiles - cut - (dead if half else 0))
        else:
            for each in range(2):

                @pl.when(half == each)
                def _():
                    act(TILE * tiles - cut - (dead if each else 0))

    mine = me - shards * home

    def own_query(piece, which, target):
        return remote(
            query_source(piece), query_slot(mine, piece), wq_own.at[piece, which], wq_recv.at[piece, mine], target
        )

    def local_query(piece, index):
        return pltpu.make_async_copy(query_source(piece), query_slot(index, piece), wq_recv.at[piece, index])

    def own_out(half, piece, which, target):
        return remote(
            out_source(half, piece), out_slot(x, c, piece), wo_own.at[half, piece, which], wo_recv.at[piece, me], target
        )

    def local_out(piece, core):
        return pltpu.make_async_copy(out_source(c, piece), out_slot(x, core, piece), wo_recv.at[piece, 2 * x + core])

    def lend_query():
        target = {"section": below, "seq": 2 * x + home}
        return remote(query_source(query_tail), aid_query(mine), wq_own.at[query_tail, 0], aq_recv.at[mine], target)

    def lend_out(half, size):
        target = {"section": below, "seq": 2 * x + half}
        source = wo_in.at[half, cut : cut + size, :]
        return remote(source, aid_out(x, c, size), wo_own.at[half, out_tail, 0], ao_recv.at[me], target)

    def own_queries(act):
        for piece in query_pieces:

            def ring():
                act(own_query(piece, 0, chip(1, home)))
                act(own_query(piece, 1, chip(-1, home)))

            if piece == query_tail:
                pl.when(~first)(ring)
                pl.when(first)(lambda: act(lend_query()))
            else:
                ring()

            @pl.when(c != home)
            def _():
                act(own_query(piece, 2, partner))

    def own_outs(act):
        for piece in out_pieces:
            for half in range(2):

                def ring():
                    act(own_out(half, piece, 0, chip(1, half)))
                    act(own_out(half, piece, 1, chip(-1, half)))

                if piece == out_tail:
                    pl.when(~first)(ring)
                else:
                    ring()
            act(own_out(other, piece, 2, partner))

    def lend_outs(act):
        @pl.when(first)
        def _():
            for half in range(2):
                halves(half, lambda size: act(lend_out(half, size)))

    def query_copy(index, sign, piece):
        slot = query_slot(index, piece)
        return remote(slot, slot, wq_relay.at[piece, index], wq_recv.at[piece, index], chip(sign, c))

    def out_copy(owner, core, sign, piece):
        slot = out_slot(owner, core, piece)
        index = 2 * owner + core
        return remote(slot, slot, wo_relay.at[piece, index], wo_recv.at[piece, index], chip(sign, c))

    def owner_of(step, sign):
        return (x - sign * step + chips) % chips

    query_hops = {1: half_chips, -1: half_chips - 1}
    out_hops = {1: half_chips - 1, -1: half_chips}

    def each_query(step, sign, act):
        owner = owner_of(step, sign)
        held = owner // half_chips == c
        for piece in query_pieces:

            @pl.when(held & ~first if piece == query_tail else held)
            def _():
                for core in range(2):
                    index = 2 * owner + core - shards * c
                    act(lambda: query_copy(index, sign, piece), step < query_hops[sign])

    def each_out(step, sign, act):
        owner = owner_of(step, sign)
        for piece in out_pieces:

            def held():
                for core in range(2):
                    act(lambda: out_copy(owner, core, sign, piece), step < out_hops[sign])

            if piece == out_tail:
                pl.when(~first)(held)
            else:
                held()

    arrivals = []
    for sign in (1, -1):
        line = [(each_query, step) for step in range(1, half_chips)] + [(each_out, 1)]
        line += [(each_query, step) for step in range(half_chips, query_hops[sign] + 1)]
        line += [(each_out, step) for step in range(2, out_hops[sign] + 1)]
        time = 0
        for kind, step in line:
            time += 5 if kind is each_query else 3
            arrivals.append((time, sign, kind, step))
    arrivals.sort(key=lambda arrival: (arrival[0], -arrival[1]))
    needed = [a for a in range(len(arrivals)) if arrivals[a][2] is each_query][-1] + 1
    ending = max(needed, len(arrivals) - 2)

    def take(low, high, act):
        for _, sign, kind, step in arrivals[low:high]:
            kind(step, sign, act)

    def relay(make, more):
        copy = make()
        copy.wait_recv()
        if more:
            copy.start()

    def settle(make, more):
        if more:
            make().wait_send()

    def steps(low, high, each, act):
        def body(step, carry):
            each(step, act)
            return carry

        lax.fori_loop(low, high, body, 0)

    def aid_query_copy(index, sign):
        slot = aid_query(index)
        return remote(slot, slot, aq_relay.at[(1 - sign) // 2, index], aq_recv.at[index], chip(sign, c))

    def aid_query_up(index):
        return remote(
            aid_query(index), query_slot(index, query_tail), aq_up.at[index], wq_recv.at[query_tail, index], up
        )

    def aid_out_copy(owner, core, sign, size):
        slot = aid_out(owner, core, size)
        index = 2 * owner + core
        return remote(slot, slot, ao_relay.at[(1 - sign) // 2, index], ao_recv.at[index], chip(sign, c))

    def aid_out_up(owner, core, size):
        index = 2 * owner + core
        target = wo.at[owner, cut : cut + size, pl.ds(pl.multiple_of(128 * core, 128), 128)]
        return remote(aid_out(owner, core, size), target, ao_up.at[index], wo_recv.at[out_tail, index], up)

    def aid_own_query(act):
        @pl.when(c == home)
        def _():
            for core in range(2):
                index = 2 * x + core - shards * c
                act(aid_query_copy(index, 1), aid_query_copy(index, -1))

    def aid_own_out(act):
        def both(size):
            for core in range(2):
                act(aid_out_copy(x, core, 1, size), aid_out_copy(x, core, -1, size))

        halves(c, both)

    def aid_each_query(step, act):
        for sign in (1, -1):
            owner = owner_of(step, sign)

            @pl.when((step <= query_hops[sign]) & (owner // half_chips == c))
            def _():
                for core in range(2):
                    index = 2 * owner + core - shards * c
                    act(aid_query_copy(index, sign), aid_query_up(index), step < query_hops[sign])

    def aid_each_out(step, act):
        for sign in (-1, 1):
            owner = owner_of(step, sign)

            @pl.when(step <= out_hops[sign])
            def _():
                def both(size):
                    for core in range(2):
                        act(
                            aid_out_copy(owner, core, sign, size), aid_out_up(owner, core, size),
                            step < out_hops[sign],
                        )

                halves(c, both)

    def aid_send(right, left):
        right.wait_recv()
        right.start()
        left.start()

    def aid_sent(right, left):
        right.wait_send()
        left.wait_send()

    def aid_relay(along, upward, more):
        along.wait_recv()
        upward.start()

        @pl.when(more)
        def _():
            along.start()

    def aid_settle(along, upward, more):
        upward.wait_send()

        @pl.when(more)
        def _():
            along.wait_send()

    def start(copy):
        copy.start()

    def sent(copy):
        copy.wait_send()

    @pl.when(last)
    def _():
        aid_own_query(aid_send)
        aid_own_out(aid_send)
        steps(1, half_chips + 1, aid_each_query, aid_relay)
        steps(1, half_chips + 1, aid_each_out, aid_relay)

    own_queries(start)
    lend_outs(start)
    for piece in query_pieces:

        @pl.when(c == home)
        def _():
            local_query(piece, mine).start()

    for piece in out_pieces:
        local_out(piece, c).start()

    rows = pl.ds(pl.multiple_of(64 * c, 64), 64)
    other_rows = pl.ds(pl.multiple_of(64 * other, 64), 64)

    def tok_remote():
        return remote(tok_in, tok.at[:, rows, :], tok_send, tok_recv.at[1], partner)

    def tok_local():
        return pltpu.make_async_copy(tok_in, tok.at[:, rows, :], tok_recv.at[0])

    h[:, width:, :] = jnp.zeros((micro, h.shape[1] - width, 128), BF16)

    @pl.when(first & (c == 1))
    def _():
        for step in range(1, chips):
            wo[(x + step) % chips, TILE * tiles - dead :, :] = jnp.zeros((dead, TILE), BF16)

    @pl.when(x == 0)
    def _():
        kv_prev[...] = jnp.zeros_like(kv_prev)

    @pl.when(first)
    def _():
        tok_remote().start()
        tok_local().start()
        tok_local().wait()
        tok_remote().wait()

        def turn(slot, carry):
            block = order_in[slot]
            for low in range(0, width, 128):
                high = min(low + 128, width)
                h[slot, low:high, :] = tok[block, :, low:high].astype(F32).T.astype(BF16)
            return carry

        lax.fori_loop(0, micro, turn, 0)

    before = 2 * (half_chips - 2)
    take(0, before, relay)
    own_outs(start)
    take(before, needed, relay)

    @pl.when(c == home)
    def _():
        for piece in query_pieces:
            for core in range(2):
                local_query(piece, 2 * x + core - shards * c).wait()

    @pl.when(first)
    def _():
        def body(step, carry):
            for sign in (1, -1):
                owner = owner_of(step, sign)

                @pl.when((step <= query_hops[sign]) & (owner // half_chips == c))
                def _():
                    for core in range(2):
                        query_copy(2 * owner + core - shards * c, sign, query_tail).wait_recv()

            return carry

        lax.fori_loop(1, half_chips + 1, body, 0)

    def finish_outs():
        for piece in out_pieces:
            for core in range(2):
                local_out(piece, core).wait()

        @pl.when(first)
        def _():
            def body(step, carry):
                for sign in (-1, 1):
                    owner = owner_of(step, sign)

                    @pl.when(step <= out_hops[sign])
                    def _():
                        def both(size):
                            for core in range(2):
                                aid_out_up(owner, core, size).wait_recv()

                        halves(c, both)

                return carry

            lax.fori_loop(1, half_chips + 1, body, 0)

    short = width - (2 * tiles - 1) * TILE

    def sized(core, k, act):
        if k < tiles - 1 or short == TILE:
            act(TILE)
        else:

            @pl.when(core == 0)
            def _():
                act(TILE)

            @pl.when(core == 1)
            def _():
                act(short)

    def h_tile(slot, k, size):
        return h.at[slot, pl.ds(pl.multiple_of(TILE * k, TILE), size), :]

    def pass_on(slot, k, size):
        return remote(
            h_new.at[slot, k, :size, :], h_tile(slot, tiles * c + k, size), h_send.at[slot, k], h_recv.at[slot, k], up
        )

    def forward(slot, k, core, size):
        piece = h_tile(slot, tiles * core + k, size)
        return remote(piece, piece, f_send.at[slot, k], f_recv.at[slot, k], partner)

    def kv_copy(slot, which):
        return remote(
            kv_own.at[slot, which], kv_prev.at[slot, which], kv_send.at[slot, which], kv_recv.at[slot, which],
            chip(1, c),
        )

    def ctx_tile(core, m):
        return pl.ds(pl.multiple_of(TILE * (ctx_tiles * core + m), TILE), TILE)

    def ctx_copy(slot, core, m):
        piece = ctx.at[slot, ctx_tile(core, m), :]
        return remote(piece, piece, c_send.at[slot, m], c_recv.at[slot, m], partner)

    def hid_columns(core, k):
        return pl.ds(pl.multiple_of(TILE * (tiles * core + k), TILE), TILE)

    def hid_local(slot, k):
        return pltpu.make_async_copy(
            stage_h.at[slot, k, rows, :], hid_out.at[slot, :, hid_columns(c, k)], oh_local.at[slot, k]
        )

    def hid_remote(slot, k, core):
        return remote(
            stage_h.at[slot, k, other_rows, :], hid_out.at[slot, :, hid_columns(core, k)],
            oh_send.at[slot, k], oh_recv.at[slot, k], partner,
        )

    def cache_columns(core, which):
        return pl.ds(pl.multiple_of(256 * which + 128 * core, 128), 128)

    def cache_source(slot, which, span):
        return kv_own.at[slot, 0, span, :] if which == 0 else stage_v.at[slot, span, :]

    def cache_local(slot, which):
        return pltpu.make_async_copy(
            cache_source(slot, which, rows), cache_out.at[slot, :, cache_columns(c, which)], oc_local.at[slot, which]
        )

    def cache_remote(slot, which, core):
        return remote(
            cache_source(slot, which, other_rows), cache_out.at[slot, :, cache_columns(core, which)],
            oc_send.at[slot, which], oc_recv.at[slot, which], partner,
        )

    key = lax.broadcasted_iota(jnp.int32, (WIN, 128), 0)
    token = lax.broadcasted_iota(jnp.int32, (WIN, 128), 1)
    lower = key <= token
    lower_pair = jnp.concatenate([lower.astype(jnp.int32)] * 2, 1) == 1

    def project(slot):
        kv_acc[...] = jnp.zeros_like(kv_acc)
        q_acc[...] = jnp.zeros_like(q_acc)
        squares = jnp.zeros((8, 128), F32)
        for own in (True, False):
            for k in range(tiles):
                core = c if own else other
                kt = tiles * core + k

                @pl.when(section > 0)
                def _():
                    def arrive(size):
                        if own:
                            pass_on(slot, k, size).wait_recv()
                            forward(slot, k, c, size).start()
                        else:
                            forward(slot, k, other, size).wait_recv()

                    sized(core, k, arrive)

                piece = h[slot, pl.ds(pl.multiple_of(TILE * kt, TILE), TILE), :]
                wide = piece.astype(F32)
                squares = squares + jnp.sum((wide * wide).reshape(TILE // 8, 8, 128), 0)
                kv_acc[...] += dot(wkv_in[kt], piece)
                if k < tiles - 1 or own:
                    q_acc[...] += dot(wq[kt], piece)
        scale = lax.rsqrt(jnp.sum(squares, 0, keepdims=True) * (1.0 / width) + EPSILON)
        cosine = cos_in[...] * scale
        sine = sin_in[...] * scale

        def rotate(first, second):
            return jnp.concatenate([first * cosine - second * sine, second * cosine + first * sine], 0)

        keys = jnp.concatenate(
            [rotate(kv_acc[64 * g : 64 * g + 32, :], kv_acc[64 * g + 32 : 64 * g + 64, :]) for g in range(2)], 0
        )
        kv_own[slot, 0] = keys.T.astype(BF16)

        @pl.when(x < chips - 1)
        def _():
            kv_copy(slot, 0).start()

        kv_own[slot, 1] = (kv_acc[128:256, :] * scale).astype(BF16)

        @pl.when(x < chips - 1)
        def _():
            kv_copy(slot, 1).start()

        q_acc[...] += dot(wq[kt], piece)
        for i in range(q.shape[0] // HEAD_DIM):
            first = q_acc[HEAD_DIM * i : HEAD_DIM * i + HALF, :]
            second = q_acc[HEAD_DIM * i + HALF : HEAD_DIM * (i + 1), :]
            q[HEAD_DIM * i : HEAD_DIM * (i + 1), :] = rotate(first, second).astype(BF16)

    def attend(slot):
        length = length_in[order_in[slot]]
        allowed_own = (WIN * x + key < length) | (key == token)
        allowed_prev = (WIN * x - WIN + key < length) & (x > 0)
        bias = jnp.where(lower, jnp.where(allowed_own, 0.0, LOW), jnp.where(allowed_prev, 0.0, LOW))
        bias = jnp.concatenate([bias, bias], 1)

        @pl.when(x > 0)
        def _():
            kv_copy(slot, 0).wait_recv()

        blank = jnp.zeros((HEAD_DIM, 256), BF16)
        ones = jnp.ones((16, 256), BF16)
        own_mask = lower_pair.astype(F32).astype(BF16)
        prev_mask = 1 - own_mask
        all_keys = jnp.concatenate([kv_own[slot, 0], kv_prev[slot, 0]], 0)
        group = shards // 2

        def raw_scores(p):
            pair = jnp.concatenate([q[128 * p : 128 * p + 64, :], q[128 * p + 64 : 128 * p + 128, :]], 1)
            return dot(all_keys, jnp.concatenate([pair, blank] if p < group else [blank, pair], 0))

        def spread(pairs):
            raw = [raw_scores(p) for p in pairs]
            out = []
            for p, both in zip(pairs, raw):
                scores = jnp.where(lower_pair, both[:WIN], both[WIN:]) + bias
                sink = jnp.concatenate([sink_in[2 * p : 2 * p + 1, :], sink_in[2 * p + 1 : 2 * p + 2, :]], 1)
                top = jnp.maximum(jnp.max(scores, 0, keepdims=True), sink)
                out.append((jnp.exp2(scores - top).astype(BF16), jnp.exp2(sink - top)))
            return out

        soft = spread(range(group))

        @pl.when(x > 0)
        def _():
            kv_copy(slot, 1).wait_recv()

        for g in range(2):
            pairs = range(group * g, group * (g + 1))
            if g > 0:
                soft = spread(pairs)
            values = jnp.concatenate(
                [kv_own[slot, 1, 64 * g : 64 * g + 64, :], kv_prev[slot, 1, 64 * g : 64 * g + 64, :]], 1
            )
            values = jnp.concatenate([values, ones], 0)
            mixed = [dot(values, jnp.concatenate([expo * own_mask, expo * prev_mask], 0)) for expo, _ in soft]
            rests = [rest for _, rest in soft]
            for p, mix, rest in zip(pairs, mixed, rests):
                total = mix[HEAD_DIM : HEAD_DIM + 1, :] + rest
                context = (mix[:HEAD_DIM, :] * (1.0 / total)).astype(BF16)
                base = pl.multiple_of(128 * shards * c + 128 * p, 128)
                ctx[slot, pl.ds(base, 64), :] = context[:, :128]
                ctx[slot, pl.ds(base + 64, 64), :] = context[:, 128:]
            for m in range(group * g // 2, group * (g + 1) // 2):
                ctx_copy(slot, c, m).start()

    def emit(slot):
        def part(core, k, m):
            return dot(wo[ctx_tiles * core + m, TILE * k : TILE * (k + 1), :], ctx[slot, ctx_tile(core, m), :])

        early, late = range(ctx_tiles // 2), range(ctx_tiles // 2, ctx_tiles)
        for k in range(tiles):
            total = part(c, k, 0)
            for m in range(1, ctx_tiles):
                total = total + part(c, k, m)
            o_acc[TILE * k : TILE * (k + 1), :] = total
        for m in early:
            ctx_copy(slot, other, m).wait_recv()
        for k in range(tiles):
            total = o_acc[TILE * k : TILE * (k + 1), :]
            for m in early:
                total = total + part(other, k, m)
            o_acc[TILE * k : TILE * (k + 1), :] = total
        for m in late:
            ctx_copy(slot, other, m).wait_recv()
        for k in range(tiles):
            total = o_acc[TILE * k : TILE * (k + 1), :]
            for m in late:
                total = total + part(other, k, m)
            row = pl.multiple_of(TILE * (tiles * c + k), TILE)
            h_new[slot, k] = (h[slot, pl.ds(row, TILE), :].astype(F32) + total).astype(BF16)

            @pl.when(section < sections - 1)
            def _():
                sized(c, k, lambda size: pass_on(slot, k, size).start())

        cache_local(slot, 0).start()
        cache_remote(slot, 0, c).start()
        stage_v[slot] = kv_own[slot, 1].astype(F32).T.astype(BF16)
        cache_local(slot, 1).start()
        cache_remote(slot, 1, c).start()
        for k in range(tiles):
            stage_h[slot, k] = h_new[slot, k].astype(F32).T.astype(BF16)
            hid_local(slot, k).start()
            hid_remote(slot, k, c).start()

    @pl.when(first)
    def _():
        project(0)

    take(needed, ending, relay)

    @pl.when(first)
    def _():
        attend(0)
        project(1)

    take(ending, len(arrivals), relay)
    finish_outs()

    @pl.when(~first)
    def _():
        project(0)
        attend(0)

    def one_slot(slot, carry):
        emit(slot)

        @pl.when(~first & (slot < micro - 1))
        def _():
            project(slot + 1)

        @pl.when(slot < micro - 1)
        def _():
            attend(slot + 1)

        @pl.when(first & (slot < micro - 2))
        def _():
            project(slot + 2)

        return carry

    lax.fori_loop(0, micro, one_slot, 0)

    def finish(slot, carry):
        for k in range(tiles):
            hid_local(slot, k).wait()
            hid_remote(slot, k, other).wait_recv()
            hid_remote(slot, k, c).wait_send()

            @pl.when(section < sections - 1)
            def _():
                sized(c, k, lambda size: pass_on(slot, k, size).wait_send())

            @pl.when(section > 0)
            def _():
                sized(c, k, lambda size: forward(slot, k, c, size).wait_send())

        for which in range(2):
            cache_local(slot, which).wait()
            cache_remote(slot, which, other).wait_recv()
            cache_remote(slot, which, c).wait_send()

            @pl.when(x < chips - 1)
            def _():
                kv_copy(slot, which).wait_send()

        for m in range(ctx_tiles):
            ctx_copy(slot, c, m).wait_send()
        return carry

    lax.fori_loop(0, micro, finish, 0)
    take(0, len(arrivals), settle)
    own_queries(sent)
    own_outs(sent)
    lend_outs(sent)

    @pl.when(last)
    def _():
        aid_own_query(aid_sent)
        aid_own_out(aid_sent)
        steps(1, half_chips + 1, aid_each_query, aid_settle)
        steps(1, half_chips + 1, aid_each_out, aid_settle)


def per_device(seqs, sections, tokens, block_order, prompt_lengths, norm_gain, w_query, w_key_value, w_out, sinks):
    micro, rows, width = tokens.shape
    padded = -(-width // (2 * TILE)) * 2 * TILE
    tiles = padded // (2 * TILE)
    shards = seqs // 2
    me = lax.axis_index("seq")
    core = me % 2
    extra = padded - width
    gain = norm_gain[0][:, None]
    kv_width = w_key_value.shape[2] // 2

    def turned(weight):
        weight = jnp.pad(weight.astype(BF16), ((0, extra), (0, 0)))
        return weight.reshape(padded // TILE, TILE, weight.shape[1]).transpose(0, 2, 1)

    wq = turned(w_query[0].astype(F32) * (gain * (HEAD_DIM**-0.5 * LOG2E)))
    pair = jnp.concatenate(
        [
            lax.dynamic_slice_in_dim(w_key_value[0], core * (kv_width // 2), kv_width // 2, 1),
            lax.dynamic_slice_in_dim(w_key_value[0], kv_width + core * (kv_width // 2), kv_width // 2, 1),
        ],
        1,
    )
    wkv = turned(pair.astype(F32) * gain)
    wo = jnp.pad(w_out[0], ((0, 0), (0, extra))).reshape(w_out.shape[1], 2, padded // 2).transpose(1, 2, 0)
    freq = jnp.exp(jnp.arange(HALF, dtype=F32) * (-2.0 * math.log(THETA) / HEAD_DIM))
    positions = (me // 2) * (2 * rows) + jnp.arange(2 * rows, dtype=jnp.int32)
    angles = freq[:, None] * positions.astype(F32)[None, :]
    heads = 2 * shards
    sink = lax.dynamic_slice_in_dim(sinks[0], core * heads, heads, 0)
    sink = jnp.broadcast_to(sink[:, None] * LOG2E, (heads, 128))

    vmem = pl.BlockSpec(memory_space=pltpu.VMEM)
    dma = pltpu.SemaphoreType.DMA
    cells = 64 * heads
    hidden, cache = pl.pallas_call(
        functools.partial(kernel, seqs, sections, micro, width),
        out_shape=(
            jax.ShapeDtypeStruct((micro, rows, padded), BF16),
            jax.ShapeDtypeStruct((micro, rows, 2 * kv_width), BF16),
        ),
        in_specs=[vmem] * 3
        + [pl.BlockSpec(memory_space=pl.ANY)]
        + [vmem] * 3
        + [pl.BlockSpec(memory_space=pltpu.SMEM)] * 2,
        out_specs=(pl.BlockSpec(memory_space=pl.ANY), pl.BlockSpec(memory_space=pl.ANY)),
        scratch_shapes=[
            pltpu.VMEM((2 * tiles, cells, TILE), BF16),
            pltpu.VMEM((shards, tiles * TILE, TILE), BF16),
            pltpu.VMEM((micro, padded, 128), BF16),
            pltpu.VMEM((micro, 128, width), BF16),
            pltpu.VMEM((256, 128), F32),
            pltpu.VMEM((cells, 128), F32),
            pltpu.VMEM((cells, 128), BF16),
            pltpu.VMEM((micro, 2, 128, 128), BF16),
            pltpu.VMEM((micro, 2, 128, 128), BF16),
            pltpu.VMEM((micro, 2 * cells, 128), BF16),
            pltpu.VMEM((tiles * TILE, 128), F32),
            pltpu.VMEM((micro, tiles, TILE, 128), BF16),
            pltpu.VMEM((micro, tiles, 128, TILE), BF16),
            pltpu.VMEM((micro, 128, 128), BF16),
            pltpu.VMEM((1, cells, TILE), BF16),
            pltpu.VMEM((shards, TILE * tiles // 2, TILE), BF16),
            dma((3, shards)), dma((3, 3)), dma((3, shards)),
            dma((2, seqs)), dma((2, 2, 3)), dma((2, seqs)),
            dma((shards,)), dma((2, shards)), dma((shards,)),
            dma((seqs,)), dma((2, seqs)), dma((seqs,)),
            dma, dma((2,)),
            dma((micro, tiles)), dma((micro, tiles)),
            dma((micro, tiles)), dma((micro, tiles)),
            dma((micro, 2)), dma((micro, 2)),
            dma((micro, shards // 2)), dma((micro, shards // 2)),
            dma((micro, tiles)), dma((micro, tiles)), dma((micro, tiles)),
            dma((micro, 2)), dma((micro, 2)), dma((micro, 2)),
        ],
        compiler_params=pltpu.CompilerParams(
            collective_id=0, has_side_effects=True, vmem_limit_bytes=50 * 1024 * 1024
        ),
    )(wq, wkv, wo, tokens, jnp.cos(angles), jnp.sin(angles), sink, prompt_lengths, block_order)
    return hidden[None, :, :, :width], cache[None]


def solution(mesh):
    in_specs = (
        P("groups", "seq", None),
        P("groups"),
        P("groups"),
        P("section", None),
        P("section", None, "seq"),
        P("section", None, None),
        P("section", "seq", None),
        P("section", None),
    )
    out_specs = (P("section", "groups", "seq", None), P("section", "groups", "seq", None))
    body = functools.partial(per_device, mesh.shape["seq"], mesh.shape["section"])
    return jax.shard_map(body, mesh=mesh, in_specs=in_specs, out_specs=out_specs, check_vma=False)
```

```python
import functools
import math

import jax
import jax.numpy as jnp
from jax import lax
from jax.experimental import pallas as pl
from jax.experimental.pallas import tpu as pltpu
from jax.sharding import PartitionSpec as P

MESH = pl.DeviceIdType.MESH
HEAD_DIM = 64
HALF = HEAD_DIM // 2
WIN = 128
TILE = 256
THETA = 150000.0
EPSILON = 1e-05
LOW = -1e30
LOG2E = math.log2(math.e)
F32 = jnp.float32
BF16 = jnp.bfloat16


def dot(a, b):
    return jnp.dot(a, b, preferred_element_type=F32)


def kernel(
    seqs, sections, micro, width,
    wq_in, wkv_in, wo_in, tok_in, cos_in, sin_in, sink_in, length_in, order_in,
    hid_out, cache_out,
    wq, wo, h, tok, kv_acc, q_acc, q, kv_own, kv_prev, ctx, o_acc, h_new, stage_h, stage_v, aq, ao,
    wq_recv, wq_own, wq_relay, wo_recv, wo_own, wo_relay,
    aq_recv, aq_relay, aq_up, ao_recv, ao_relay, ao_up,
    tok_send, tok_recv, h_send, h_recv, f_send, f_recv, kv_send, kv_recv, c_send, c_recv,
    oh_local, oh_send, oh_recv, oc_local, oc_send, oc_recv,
):
    chips = seqs // 2
    half_chips = chips // 2
    shards = seqs // 2
    tiles = h.shape[1] // (2 * TILE)
    cut = TILE * tiles - ao.shape[1]
    ctx_tiles = shards // 2
    me = lax.axis_index("seq")
    section = lax.axis_index("section")
    x = me // 2
    c = me % 2
    other = 1 - c
    partner = {"seq": 2 * x + other}

    def chip(step, core):
        return {"seq": 2 * ((x + step + chips) % chips) + core}

    def remote(src, dst, send, recv, target):
        return pltpu.make_async_remote_copy(
            src_ref=src, dst_ref=dst, send_sem=send, recv_sem=recv, device_id=target, device_id_type=MESH
        )

    first = section == 0
    last = section == sections - 1
    above = (section + 1) % sections
    below = (section + sections - 1) % sections
    up = {"section": above}
    barrier = pltpu.get_barrier_semaphore()
    greeted = [partner] + [chip(step, core) for step in (1, -1) for core in range(2)]
    greeted += [{"section": level, "seq": 2 * x + core} for level in (above, below) for core in range(2)]
    for target in greeted:
        pl.semaphore_signal(barrier, inc=1, device_id=target, device_id_type=MESH)
    pl.semaphore_wait(barrier, len(greeted))

    home = x // half_chips
    query_cuts = (0, tiles, 2 * tiles - 1, 2 * tiles)
    out_cuts = (0, cut, TILE * tiles)
    dead = h.shape[1] - width
    query_pieces, out_pieces = range(3), range(2)
    query_tail, out_tail = 2, 1

    def query_slot(index, piece):
        lo, hi = query_cuts[piece : piece + 2]
        return wq.at[lo:hi, pl.ds(pl.multiple_of(128 * index, 128), 128), :]

    def out_slot(owner, core, piece):
        lo, hi = out_cuts[piece : piece + 2]
        return wo.at[owner, lo:hi, pl.ds(pl.multiple_of(128 * core, 128), 128)]

    def query_source(piece):
        return wq_in.at[query_cuts[piece] : query_cuts[piece + 1]]

    def out_source(half, piece):
        return wo_in.at[half, out_cuts[piece] : out_cuts[piece + 1], :]

    def aid_query(index):
        return aq.at[:, pl.ds(pl.multiple_of(128 * index, 128), 128), :]

    def aid_out(owner, core, size):
        return ao.at[owner, :size, pl.ds(pl.multiple_of(128 * core, 128), 128)]

    def halves(half, act):
        if isinstance(half, int):
            act(TILE * tiles - cut - (dead if half else 0))
        else:
            for each in range(2):

                @pl.when(half == each)
                def _():
                    act(TILE * tiles - cut - (dead if each else 0))

    mine = me - shards * home

    def own_query(piece, which, target):
        return remote(
            query_source(piece), query_slot(mine, piece), wq_own.at[piece, which], wq_recv.at[piece, mine], target
        )

    def local_query(piece, index):
        return pltpu.make_async_copy(query_source(piece), query_slot(index, piece), wq_recv.at[piece, index])

    def own_out(half, piece, which, target):
        return remote(
            out_source(half, piece), out_slot(x, c, piece), wo_own.at[half, piece, which], wo_recv.at[piece, me], target
        )

    def local_out(piece, core):
        return pltpu.make_async_copy(out_source(c, piece), out_slot(x, core, piece), wo_recv.at[piece, 2 * x + core])

    def lend_query():
        target = {"section": below, "seq": 2 * x + home}
        return remote(query_source(query_tail), aid_query(mine), wq_own.at[query_tail, 0], aq_recv.at[mine], target)

    def lend_out(half, size):
        target = {"section": below, "seq": 2 * x + half}
        source = wo_in.at[half, cut : cut + size, :]
        return remote(source, aid_out(x, c, size), wo_own.at[half, out_tail, 0], ao_recv.at[me], target)

    def own_queries(act):
        for piece in query_pieces:

            def ring():
                act(own_query(piece, 0, chip(1, home)))
                act(own_query(piece, 1, chip(-1, home)))

            if piece == query_tail:
                pl.when(~first)(ring)
                pl.when(first)(lambda: act(lend_query()))
            else:
                ring()

            @pl.when(c != home)
            def _():
                act(own_query(piece, 2, partner))

    def own_outs(act):
        for piece in out_pieces:
            for half in range(2):

                def ring():
                    act(own_out(half, piece, 0, chip(1, half)))
                    act(own_out(half, piece, 1, chip(-1, half)))

                if piece == out_tail:
                    pl.when(~first)(ring)
                else:
                    ring()
            act(own_out(other, piece, 2, partner))

    def lend_outs(act):
        @pl.when(first)
        def _():
            for half in range(2):
                halves(half, lambda size: act(lend_out(half, size)))

    def query_copy(index, sign, piece):
        slot = query_slot(index, piece)
        return remote(slot, slot, wq_relay.at[piece, index], wq_recv.at[piece, index], chip(sign, c))

    def out_copy(owner, core, sign, piece):
        slot = out_slot(owner, core, piece)
        index = 2 * owner + core
        return remote(slot, slot, wo_relay.at[piece, index], wo_recv.at[piece, index], chip(sign, c))

    def owner_of(step, sign):
        return (x - sign * step + chips) % chips

    query_hops = {1: half_chips, -1: half_chips - 1}
    out_hops = {1: half_chips - 1, -1: half_chips}

    def each_query(step, sign, act):
        owner = owner_of(step, sign)
        held = owner // half_chips == c
        for piece in query_pieces:

            @pl.when(held & ~first if piece == query_tail else held)
            def _():
                for core in range(2):
                    index = 2 * owner + core - shards * c
                    act(lambda: query_copy(index, sign, piece), step < query_hops[sign])

    def each_out(step, sign, act):
        owner = owner_of(step, sign)
        for piece in out_pieces:

            def held():
                for core in range(2):
                    act(lambda: out_copy(owner, core, sign, piece), step < out_hops[sign])

            if piece == out_tail:
                pl.when(~first)(held)
            else:
                held()

    arrivals = []
    for sign in (1, -1):
        line = [(each_query, step) for step in range(1, half_chips)] + [(each_out, 1)]
        line += [(each_query, step) for step in range(half_chips, query_hops[sign] + 1)]
        line += [(each_out, step) for step in range(2, out_hops[sign] + 1)]
        time = 0
        for kind, step in line:
            time += 5 if kind is each_query else 3
            arrivals.append((time, sign, kind, step))
    arrivals.sort(key=lambda arrival: (arrival[0], -arrival[1]))
    needed = [a for a in range(len(arrivals)) if arrivals[a][2] is each_query][-1] + 1
    ending = max(needed, len(arrivals) - 2)

    def take(low, high, act):
        for _, sign, kind, step in arrivals[low:high]:
            kind(step, sign, act)

    def relay(make, more):
        copy = make()
        copy.wait_recv()
        if more:
            copy.start()

    def settle(make, more):
        if more:
            make().wait_send()

    def steps(low, high, each, act):
        def body(step, carry):
            each(step, act)
            return carry

        lax.fori_loop(low, high, body, 0)

    def aid_query_copy(index, sign):
        slot = aid_query(index)
        return remote(slot, slot, aq_relay.at[(1 - sign) // 2, index], aq_recv.at[index], chip(sign, c))

    def aid_query_up(index):
        return remote(
            aid_query(index), query_slot(index, query_tail), aq_up.at[index], wq_recv.at[query_tail, index], up
        )

    def aid_out_copy(owner, core, sign, size):
        slot = aid_out(owner, core, size)
        index = 2 * owner + core
        return remote(slot, slot, ao_relay.at[(1 - sign) // 2, index], ao_recv.at[index], chip(sign, c))

    def aid_out_up(owner, core, size):
        index = 2 * owner + core
        target = wo.at[owner, cut : cut + size, pl.ds(pl.multiple_of(128 * core, 128), 128)]
        return remote(aid_out(owner, core, size), target, ao_up.at[index], wo_recv.at[out_tail, index], up)

    def aid_own_query(act):
        @pl.when(c == home)
        def _():
            for core in range(2):
                index = 2 * x + core - shards * c
                act(aid_query_copy(index, 1), aid_query_copy(index, -1))

    def aid_own_out(act):
        def both(size):
            for core in range(2):
                act(aid_out_copy(x, core, 1, size), aid_out_copy(x, core, -1, size))

        halves(c, both)

    def aid_each_query(step, act):
        for sign in (1, -1):
            owner = owner_of(step, sign)

            @pl.when((step <= query_hops[sign]) & (owner // half_chips == c))
            def _():
                for core in range(2):
                    index = 2 * owner + core - shards * c
                    act(aid_query_copy(index, sign), aid_query_up(index), step < query_hops[sign])

    def aid_each_out(step, act):
        for sign in (-1, 1):
            owner = owner_of(step, sign)

            @pl.when(step <= out_hops[sign])
            def _():
                def both(size):
                    for core in range(2):
                        act(
                            aid_out_copy(owner, core, sign, size), aid_out_up(owner, core, size),
                            step < out_hops[sign],
                        )

                halves(c, both)

    def aid_send(right, left):
        right.wait_recv()
        right.start()
        left.start()

    def aid_sent(right, left):
        right.wait_send()
        left.wait_send()

    def aid_relay(along, upward, more):
        along.wait_recv()
        upward.start()

        @pl.when(more)
        def _():
            along.start()

    def aid_settle(along, upward, more):
        upward.wait_send()

        @pl.when(more)
        def _():
            along.wait_send()

    def start(copy):
        copy.start()

    def sent(copy):
        copy.wait_send()

    @pl.when(last)
    def _():
        aid_own_query(aid_send)
        aid_own_out(aid_send)
        steps(1, half_chips + 1, aid_each_query, aid_relay)
        steps(1, half_chips + 1, aid_each_out, aid_relay)

    own_queries(start)
    lend_outs(start)
    for piece in query_pieces:

        @pl.when(c == home)
        def _():
            local_query(piece, mine).start()

    for piece in out_pieces:
        local_out(piece, c).start()

    rows = pl.ds(pl.multiple_of(64 * c, 64), 64)
    other_rows = pl.ds(pl.multiple_of(64 * other, 64), 64)

    def tok_remote():
        return remote(tok_in, tok.at[:, rows, :], tok_send, tok_recv.at[1], partner)

    def tok_local():
        return pltpu.make_async_copy(tok_in, tok.at[:, rows, :], tok_recv.at[0])

    h[:, width:, :] = jnp.zeros((micro, h.shape[1] - width, 128), BF16)

    @pl.when(first & (c == 1))
    def _():
        for step in range(1, chips):
            wo[(x + step) % chips, TILE * tiles - dead :, :] = jnp.zeros((dead, TILE), BF16)

    @pl.when(x == 0)
    def _():
        kv_prev[...] = jnp.zeros_like(kv_prev)

    @pl.when(first)
    def _():
        tok_remote().start()
        tok_local().start()
        tok_local().wait()
        tok_remote().wait()

        def turn(slot, carry):
            block = order_in[slot]
            for low in range(0, width, 128):
                high = min(low + 128, width)
                h[slot, low:high, :] = tok[block, :, low:high].astype(F32).T.astype(BF16)
            return carry

        lax.fori_loop(0, micro, turn, 0)

    before = 2 * (half_chips - 2)
    take(0, before, relay)
    own_outs(start)
    take(before, needed, relay)

    @pl.when(c == home)
    def _():
        for piece in query_pieces:
            for core in range(2):
                local_query(piece, 2 * x + core - shards * c).wait()

    @pl.when(first)
    def _():
        def body(step, carry):
            for sign in (1, -1):
                owner = owner_of(step, sign)

                @pl.when((step <= query_hops[sign]) & (owner // half_chips == c))
                def _():
                    for core in range(2):
                        query_copy(2 * owner + core - shards * c, sign, query_tail).wait_recv()

            return carry

        lax.fori_loop(1, half_chips + 1, body, 0)

    def finish_outs():
        for piece in out_pieces:
            for core in range(2):
                local_out(piece, core).wait()

        @pl.when(first)
        def _():
            def body(step, carry):
                for sign in (-1, 1):
                    owner = owner_of(step, sign)

                    @pl.when(step <= out_hops[sign])
                    def _():
                        def both(size):
                            for core in range(2):
                                aid_out_up(owner, core, size).wait_recv()

                        halves(c, both)

                return carry

            lax.fori_loop(1, half_chips + 1, body, 0)

    short = width - (2 * tiles - 1) * TILE

    def sized(core, k, act):
        if k < tiles - 1 or short == TILE:
            act(TILE)
        else:

            @pl.when(core == 0)
            def _():
                act(TILE)

            @pl.when(core == 1)
            def _():
                act(short)

    def h_tile(slot, k, size):
        return h.at[slot, pl.ds(pl.multiple_of(TILE * k, TILE), size), :]

    def pass_on(slot, k, size):
        return remote(
            h_new.at[slot, k, :size, :], h_tile(slot, tiles * c + k, size), h_send.at[slot, k], h_recv.at[slot, k], up
        )

    def forward(slot, k, core, size):
        piece = h_tile(slot, tiles * core + k, size)
        return remote(piece, piece, f_send.at[slot, k], f_recv.at[slot, k], partner)

    def kv_copy(slot, which):
        return remote(
            kv_own.at[slot, which], kv_prev.at[slot, which], kv_send.at[slot, which], kv_recv.at[slot, which],
            chip(1, c),
        )

    def ctx_tile(core, m):
        return pl.ds(pl.multiple_of(TILE * (ctx_tiles * core + m), TILE), TILE)

    def ctx_copy(slot, core, m):
        piece = ctx.at[slot, ctx_tile(core, m), :]
        return remote(piece, piece, c_send.at[slot, m], c_recv.at[slot, m], partner)

    def hid_columns(core, k):
        return pl.ds(pl.multiple_of(TILE * (tiles * core + k), TILE), TILE)

    def hid_local(slot, k):
        return pltpu.make_async_copy(
            stage_h.at[slot, k, rows, :], hid_out.at[slot, :, hid_columns(c, k)], oh_local.at[slot, k]
        )

    def hid_remote(slot, k, core):
        return remote(
            stage_h.at[slot, k, other_rows, :], hid_out.at[slot, :, hid_columns(core, k)],
            oh_send.at[slot, k], oh_recv.at[slot, k], partner,
        )

    def cache_columns(core, which):
        return pl.ds(pl.multiple_of(256 * which + 128 * core, 128), 128)

    def cache_source(slot, which, span):
        return kv_own.at[slot, 0, span, :] if which == 0 else stage_v.at[slot, span, :]

    def cache_local(slot, which):
        return pltpu.make_async_copy(
            cache_source(slot, which, rows), cache_out.at[slot, :, cache_columns(c, which)], oc_local.at[slot, which]
        )

    def cache_remote(slot, which, core):
        return remote(
            cache_source(slot, which, other_rows), cache_out.at[slot, :, cache_columns(core, which)],
            oc_send.at[slot, which], oc_recv.at[slot, which], partner,
        )

    key = lax.broadcasted_iota(jnp.int32, (WIN, 128), 0)
    token = lax.broadcasted_iota(jnp.int32, (WIN, 128), 1)
    lower = key <= token
    lower_pair = jnp.concatenate([lower.astype(jnp.int32)] * 2, 1) == 1

    def project(slot):
        kv_acc[...] = jnp.zeros_like(kv_acc)
        q_acc[...] = jnp.zeros_like(q_acc)
        squares = jnp.zeros((8, 128), F32)
        for own in (True, False):
            for k in range(tiles):
                core = c if own else other
                kt = tiles * core + k

                @pl.when(section > 0)
                def _():
                    def arrive(size):
                        if own:
                            pass_on(slot, k, size).wait_recv()
                            forward(slot, k, c, size).start()
                        else:
                            forward(slot, k, other, size).wait_recv()

                    sized(core, k, arrive)

                piece = h[slot, pl.ds(pl.multiple_of(TILE * kt, TILE), TILE), :]
                wide = piece.astype(F32)
                squares = squares + jnp.sum((wide * wide).reshape(TILE // 8, 8, 128), 0)
                kv_acc[...] += dot(wkv_in[kt], piece)
                if k < tiles - 1 or own:
                    q_acc[...] += dot(wq[kt], piece)
        scale = lax.rsqrt(jnp.sum(squares, 0, keepdims=True) * (1.0 / width) + EPSILON)
        cosine = cos_in[...] * scale
        sine = sin_in[...] * scale

        def rotate(first, second):
            return jnp.concatenate([first * cosine - second * sine, second * cosine + first * sine], 0)

        keys = jnp.concatenate(
            [rotate(kv_acc[64 * g : 64 * g + 32, :], kv_acc[64 * g + 32 : 64 * g + 64, :]) for g in range(2)], 0
        )
        kv_own[slot, 0] = keys.T.astype(BF16)

        @pl.when(x < chips - 1)
        def _():
            kv_copy(slot, 0).start()

        kv_own[slot, 1] = (kv_acc[128:256, :] * scale).astype(BF16)

        @pl.when(x < chips - 1)
        def _():
            kv_copy(slot, 1).start()

        q_acc[...] += dot(wq[kt], piece)
        for i in range(q.shape[0] // HEAD_DIM):
            first = q_acc[HEAD_DIM * i : HEAD_DIM * i + HALF, :]
            second = q_acc[HEAD_DIM * i + HALF : HEAD_DIM * (i + 1), :]
            q[HEAD_DIM * i : HEAD_DIM * (i + 1), :] = rotate(first, second).astype(BF16)

    def attend(slot):
        length = length_in[order_in[slot]]
        allowed_own = (WIN * x + key < length) | (key == token)
        allowed_prev = (WIN * x - WIN + key < length) & (x > 0)
        bias = jnp.where(lower, jnp.where(allowed_own, 0.0, LOW), jnp.where(allowed_prev, 0.0, LOW))
        bias = jnp.concatenate([bias, bias], 1)

        @pl.when(x > 0)
        def _():
            kv_copy(slot, 0).wait_recv()

        blank = jnp.zeros((HEAD_DIM, 256), BF16)
        ones = jnp.ones((16, 256), BF16)
        own_mask = lower_pair.astype(F32).astype(BF16)
        prev_mask = 1 - own_mask
        all_keys = jnp.concatenate([kv_own[slot, 0], kv_prev[slot, 0]], 0)
        group = shards // 2

        def raw_scores(p):
            pair = jnp.concatenate([q[128 * p : 128 * p + 64, :], q[128 * p + 64 : 128 * p + 128, :]], 1)
            return dot(all_keys, jnp.concatenate([pair, blank] if p < group else [blank, pair], 0))

        def spread(pairs):
            raw = [raw_scores(p) for p in pairs]
            out = []
            for p, both in zip(pairs, raw):
                scores = jnp.where(lower_pair, both[:WIN], both[WIN:]) + bias
                sink = jnp.concatenate([sink_in[2 * p : 2 * p + 1, :], sink_in[2 * p + 1 : 2 * p + 2, :]], 1)
                top = jnp.maximum(jnp.max(scores, 0, keepdims=True), sink)
                out.append((jnp.exp2(scores - top).astype(BF16), jnp.exp2(sink - top)))
            return out

        soft = spread(range(group))

        @pl.when(x > 0)
        def _():
            kv_copy(slot, 1).wait_recv()

        for g in range(2):
            pairs = range(group * g, group * (g + 1))
            if g > 0:
                soft = spread(pairs)
            values = jnp.concatenate(
                [kv_own[slot, 1, 64 * g : 64 * g + 64, :], kv_prev[slot, 1, 64 * g : 64 * g + 64, :]], 1
            )
            values = jnp.concatenate([values, ones], 0)
            mixed = [dot(values, jnp.concatenate([expo * own_mask, expo * prev_mask], 0)) for expo, _ in soft]
            rests = [rest for _, rest in soft]
            for p, mix, rest in zip(pairs, mixed, rests):
                total = mix[HEAD_DIM : HEAD_DIM + 1, :] + rest
                context = (mix[:HEAD_DIM, :] * (1.0 / total)).astype(BF16)
                base = pl.multiple_of(128 * shards * c + 128 * p, 128)
                ctx[slot, pl.ds(base, 64), :] = context[:, :128]
                ctx[slot, pl.ds(base + 64, 64), :] = context[:, 128:]
            for m in range(group * g // 2, group * (g + 1) // 2):
                ctx_copy(slot, c, m).start()

    def emit(slot):
        def part(core, k, m):
            return dot(wo[ctx_tiles * core + m, TILE * k : TILE * (k + 1), :], ctx[slot, ctx_tile(core, m), :])

        early, late = range(ctx_tiles // 2), range(ctx_tiles // 2, ctx_tiles)
        for k in range(tiles):
            total = part(c, k, 0)
            for m in range(1, ctx_tiles):
                total = total + part(c, k, m)
            o_acc[TILE * k : TILE * (k + 1), :] = total
        for m in early:
            ctx_copy(slot, other, m).wait_recv()
        for k in range(tiles):
            total = o_acc[TILE * k : TILE * (k + 1), :]
            for m in early:
                total = total + part(other, k, m)
            o_acc[TILE * k : TILE * (k + 1), :] = total
        for m in late:
            ctx_copy(slot, other, m).wait_recv()
        for k in range(tiles):
            total = o_acc[TILE * k : TILE * (k + 1), :]
            for m in late:
                total = total + part(other, k, m)
            row = pl.multiple_of(TILE * (tiles * c + k), TILE)
            h_new[slot, k] = (h[slot, pl.ds(row, TILE), :].astype(F32) + total).astype(BF16)

            @pl.when(section < sections - 1)
            def _():
                sized(c, k, lambda size: pass_on(slot, k, size).start())

        cache_local(slot, 0).start()
        cache_remote(slot, 0, c).start()
        stage_v[slot] = kv_own[slot, 1].astype(F32).T.astype(BF16)
        cache_local(slot, 1).start()
        cache_remote(slot, 1, c).start()
        for k in range(tiles):
            stage_h[slot, k] = h_new[slot, k].astype(F32).T.astype(BF16)
            hid_local(slot, k).start()
            hid_remote(slot, k, c).start()

    @pl.when(first)
    def _():
        project(0)

    take(needed, ending, relay)

    @pl.when(~first)
    def _():
        project(0)

    attend(0)

    @pl.when(first)
    def _():
        project(1)

    take(ending, len(arrivals), relay)
    finish_outs()

    def one_slot(slot, carry):
        emit(slot)

        @pl.when(~first & (slot < micro - 1))
        def _():
            project(slot + 1)

        @pl.when(slot < micro - 1)
        def _():
            attend(slot + 1)

        @pl.when(first & (slot < micro - 2))
        def _():
            project(slot + 2)

        return carry

    lax.fori_loop(0, micro, one_slot, 0)

    def finish(slot, carry):
        for k in range(tiles):
            hid_local(slot, k).wait()
            hid_remote(slot, k, other).wait_recv()
            hid_remote(slot, k, c).wait_send()

            @pl.when(section < sections - 1)
            def _():
                sized(c, k, lambda size: pass_on(slot, k, size).wait_send())

            @pl.when(section > 0)
            def _():
                sized(c, k, lambda size: forward(slot, k, c, size).wait_send())

        for which in range(2):
            cache_local(slot, which).wait()
            cache_remote(slot, which, other).wait_recv()
            cache_remote(slot, which, c).wait_send()

            @pl.when(x < chips - 1)
            def _():
                kv_copy(slot, which).wait_send()

        for m in range(ctx_tiles):
            ctx_copy(slot, c, m).wait_send()
        return carry

    lax.fori_loop(0, micro, finish, 0)
    take(0, len(arrivals), settle)
    own_queries(sent)
    own_outs(sent)
    lend_outs(sent)

    @pl.when(last)
    def _():
        aid_own_query(aid_sent)
        aid_own_out(aid_sent)
        steps(1, half_chips + 1, aid_each_query, aid_settle)
        steps(1, half_chips + 1, aid_each_out, aid_settle)


def per_device(seqs, sections, tokens, block_order, prompt_lengths, norm_gain, w_query, w_key_value, w_out, sinks):
    micro, rows, width = tokens.shape
    padded = -(-width // (2 * TILE)) * 2 * TILE
    tiles = padded // (2 * TILE)
    shards = seqs // 2
    me = lax.axis_index("seq")
    core = me % 2
    extra = padded - width
    gain = norm_gain[0][:, None]
    kv_width = w_key_value.shape[2] // 2

    def turned(weight):
        weight = jnp.pad(weight.astype(BF16), ((0, extra), (0, 0)))
        return weight.reshape(padded // TILE, TILE, weight.shape[1]).transpose(0, 2, 1)

    wq = turned(w_query[0].astype(F32) * (gain * (HEAD_DIM**-0.5 * LOG2E)))
    pair = jnp.concatenate(
        [
            lax.dynamic_slice_in_dim(w_key_value[0], core * (kv_width // 2), kv_width // 2, 1),
            lax.dynamic_slice_in_dim(w_key_value[0], kv_width + core * (kv_width // 2), kv_width // 2, 1),
        ],
        1,
    )
    wkv = turned(pair.astype(F32) * gain)
    wo = jnp.pad(w_out[0], ((0, 0), (0, extra))).reshape(w_out.shape[1], 2, padded // 2).transpose(1, 2, 0)
    freq = jnp.exp(jnp.arange(HALF, dtype=F32) * (-2.0 * math.log(THETA) / HEAD_DIM))
    positions = (me // 2) * (2 * rows) + jnp.arange(2 * rows, dtype=jnp.int32)
    angles = freq[:, None] * positions.astype(F32)[None, :]
    heads = 2 * shards
    sink = lax.dynamic_slice_in_dim(sinks[0], core * heads, heads, 0)
    sink = jnp.broadcast_to(sink[:, None] * LOG2E, (heads, 128))

    vmem = pl.BlockSpec(memory_space=pltpu.VMEM)
    dma = pltpu.SemaphoreType.DMA
    cells = 64 * heads
    hidden, cache = pl.pallas_call(
        functools.partial(kernel, seqs, sections, micro, width),
        out_shape=(
            jax.ShapeDtypeStruct((micro, rows, padded), BF16),
            jax.ShapeDtypeStruct((micro, rows, 2 * kv_width), BF16),
        ),
        in_specs=[vmem] * 7 + [pl.BlockSpec(memory_space=pltpu.SMEM)] * 2,
        out_specs=(pl.BlockSpec(memory_space=pl.ANY), pl.BlockSpec(memory_space=pl.ANY)),
        scratch_shapes=[
            pltpu.VMEM((2 * tiles, cells, TILE), BF16),
            pltpu.VMEM((shards, tiles * TILE, TILE), BF16),
            pltpu.VMEM((micro, padded, 128), BF16),
            pltpu.VMEM((micro, 128, width), BF16),
            pltpu.VMEM((256, 128), F32),
            pltpu.VMEM((cells, 128), F32),
            pltpu.VMEM((cells, 128), BF16),
            pltpu.VMEM((micro, 2, 128, 128), BF16),
            pltpu.VMEM((micro, 2, 128, 128), BF16),
            pltpu.VMEM((micro, 2 * cells, 128), BF16),
            pltpu.VMEM((tiles * TILE, 128), F32),
            pltpu.VMEM((micro, tiles, TILE, 128), BF16),
            pltpu.VMEM((micro, tiles, 128, TILE), BF16),
            pltpu.VMEM((micro, 128, 128), BF16),
            pltpu.VMEM((1, cells, TILE), BF16),
            pltpu.VMEM((shards, TILE * tiles // 2, TILE), BF16),
            dma((3, shards)), dma((3, 3)), dma((3, shards)),
            dma((2, seqs)), dma((2, 2, 3)), dma((2, seqs)),
            dma((shards,)), dma((2, shards)), dma((shards,)),
            dma((seqs,)), dma((2, seqs)), dma((seqs,)),
            dma, dma((2,)),
            dma((micro, tiles)), dma((micro, tiles)),
            dma((micro, tiles)), dma((micro, tiles)),
            dma((micro, 2)), dma((micro, 2)),
            dma((micro, shards // 2)), dma((micro, shards // 2)),
            dma((micro, tiles)), dma((micro, tiles)), dma((micro, tiles)),
            dma((micro, 2)), dma((micro, 2)), dma((micro, 2)),
        ],
        compiler_params=pltpu.CompilerParams(
            collective_id=0, has_side_effects=True, vmem_limit_bytes=50 * 1024 * 1024
        ),
    )(wq, wkv, wo, tokens, jnp.cos(angles), jnp.sin(angles), sink, prompt_lengths, block_order)
    return hidden[None, :, :, :width], cache[None]


def solution(mesh):
    in_specs = (
        P("groups", "seq", None),
        P("groups"),
        P("groups"),
        P("section", None),
        P("section", None, "seq"),
        P("section", None, None),
        P("section", "seq", None),
        P("section", None),
    )
    out_specs = (P("section", "groups", "seq", None), P("section", "groups", "seq", None))
    body = functools.partial(per_device, mesh.shape["seq"], mesh.shape["section"])
    return jax.shard_map(body, mesh=mesh, in_specs=in_specs, out_specs=out_specs, check_vma=False)
```
